32 devices in a mesh: seq: 4 (over y, x), exp: 8 (over z, core).
Axes of the slice: x: 2, y: 2, z: 4, core: 2. Of those that a mesh axis runs over, the one named last changes fastest.
Arguments:
- queries: bfloat16 [4096, 3072], P(('seq', 'exp')), may hold values from -123 to 123
- keys: bfloat16 [4096, 512], P(('seq', 'exp')), may hold values from -6 to 6
- values: bfloat16 [4096, 512], P(('seq', 'exp')), may hold values from -9 to 9
- residual: bfloat16 [4096, 6144], P(('seq', 'exp')), may hold values from -51 to 51
- proj_weight: bfloat16 [3072, 6144], P('seq', 'exp'), may hold values from -0.109375 to 0.109375
- norm_gain: bfloat16 [6144], replicated, may hold values from 0.099609375 to 1.8984375
- router: bfloat16 [6144, 8], replicated, may hold values from -0.078125 to 0.078125
- expert_ids: int32 [4096, 2], P(('seq', 'exp')), may hold values from 0 to 7, all different within a row; in each aligned block of 128 rows (0 to 127, 128 to 255, ...) at most 33 rows name the same one
- u_gate_up: bfloat16 [8, 6144, 1024], P('exp'), may hold values from -0.078125 to 0.078125
- v_gate_up: bfloat16 [8, 2, 512, 8192], P('exp'), may hold values from -0.25 to 0.25
- u_down: bfloat16 [8, 8192, 512], P('exp'), may hold values from -0.0625 to 0.0625
- v_down: bfloat16 [8, 512, 6144], P('exp'), may hold values from -0.25 to 0.25
Outputs:
- layer_out: bfloat16 [4096, 6144], P(('seq', 'exp'))
The draws below stay inside these ranges and needn't reach their ends.
Inputs may be any that keep to these rules, and one draw needn't show every extreme that they name: `expert_ids`: the two experts of a token differ. Among the tokens of one device no expert is named more than 33 times, and in some devices' tokens some expert is named exactly 33 times.
All inputs are finite; a program needn't handle non-finite values.
Results may differ from the reference program's by a relative error of at most 0.02.
Values may be sent and summed in bfloat16 or wider, within the bound.
A program may use at most 192 MiB of HBM per device.

```python
import math
import jax
import jax.numpy as jnp
import numpy as np
from jax import lax

D = 6144
HEADS = 24
KV_HEADS = 4
HEAD_DIM = 128
EXPERTS = 8
TOP = 2
RANK = 512
FF = 8192
TOK_DEV = 128
CAP = 33
PIECES = 1
TOKENS = 4096


def draw_queries(key, part):
    noise_draw = jax.random.normal(jax.random.fold_in(key, 902), (TOKENS, HEADS, HEAD_DIM), jnp.float32)
    noise_draw = jnp.clip(noise_draw, -6.0, 6.0)
    return noise_draw.reshape(TOKENS, HEADS * HEAD_DIM).astype(jnp.bfloat16)


def draw_keys(key, part):
    noise_draw = jax.random.normal(jax.random.fold_in(key, 903), (TOKENS, KV_HEADS, HEAD_DIM), jnp.float32)
    noise_draw = jnp.clip(noise_draw, -6.0, 6.0)
    return noise_draw.reshape(TOKENS, KV_HEADS * HEAD_DIM).astype(jnp.bfloat16)


def draw_values(key, part):
    noise_draw = jax.random.normal(jax.random.fold_in(key, 904), (TOKENS, KV_HEADS * HEAD_DIM), jnp.float32)
    noise_draw = jnp.clip(noise_draw, -6.0, 6.0)
    levels = jax.random.normal(jax.random.fold_in(key, 905), (TOKENS // 256, KV_HEADS * HEAD_DIM), jnp.float32)
    levels = jnp.clip(levels, -3.0, 3.0)
    level_rows = jnp.repeat(levels, 256, axis=0)
    return (noise_draw + level_rows).astype(jnp.bfloat16)


def draw_residual(key, part):
    noise_draw = jax.random.normal(jax.random.fold_in(key, 907), (TOKENS, D), jnp.float32)
    noise_draw = jnp.clip(noise_draw, -4.0, 4.0)
    return noise_draw.astype(jnp.bfloat16)


def block_levels(own_key, dims, shards, least, top_value):
    gain = 1.0
    for dim, parts in shards:
        heights = jax.random.uniform(jax.random.fold_in(jax.random.fold_in(own_key, 6), dim), (parts,), jnp.float32, least / len(shards), top_value / len(shards))
        gain = gain * jnp.repeat(jnp.exp(heights), dims[dim] // parts).reshape((-1,) + (1,) * (len(dims) - 1 - dim))
    return gain


def assign_block(own_key, own, number, rows, number_of, top, limit, slope):
    ranking = jax.random.permutation(own_key, number_of)
    heavy_load, ordinary = load_shares(number_of, rows * top, limit, slope, True), load_shares(number_of, rows * top, limit, slope, False)
    places = jnp.arange(number_of)

    def named(lengths, turn):
        used = int((lengths > 0).sum())
        fixed = max(1, used // 4)
        passed = fixed + (places - fixed + turn * (used - fixed)) % max(1, number_of - fixed)
        return jnp.zeros((number_of,), jnp.int32).at[ranking[jnp.where(places < fixed, places, passed)]].set(jnp.asarray(lengths, jnp.int32))

    lengths = jnp.where(number % 4 == 0, named(heavy_load, number // 4), named(ordinary, number - number // 4 - 1))
    mixed = jax.random.permutation(jax.random.fold_in(own, 3), number_of)
    giver, sink = mixed[0:number_of // 2 * 2:2], mixed[1:number_of // 2 * 2:2]
    slack = jnp.minimum(lengths[giver] - 1, limit - lengths[sink]) // 2
    slack = jnp.where((giver == ranking[0]) | (sink == ranking[0]) | (lengths[sink] == 0), 0, jnp.maximum(slack, 0))
    passed = jax.random.randint(jax.random.fold_in(own, 4), (number_of // 2,), 0, 1 << 20) % (slack + 1)
    lengths = lengths.at[giver].add(-passed).at[sink].add(passed)
    items = jnp.searchsorted(jnp.cumsum(lengths), jnp.arange(rows * top), side="right").astype(jnp.int32)
    grid = items.reshape(top, rows).T
    grid = grid[jax.random.permutation(jax.random.fold_in(own, 1), rows)]
    turn = jax.random.randint(jax.random.fold_in(own, 2), (rows, 1), 0, top)
    return jnp.take_along_axis(grid, (jnp.arange(top)[None, :] + turn) % top, axis=1)


def load_shares(amount, total, most, slope, full):
    weights = [(1 << 20) // math.isqrt(rank ** slope) + 1 for rank in range(1, amount + 1)]
    largest = most if full else min(most, max(-(-total // amount), total * weights[0] // sum(weights)))
    least = 1 if total - largest >= amount - 1 else 0
    given, surplus = [largest] + [least] * (amount - 1), total - largest - least * (amount - 1)
    while surplus > 0:
        movable = [i for i in range(1, amount) if given[i] < largest] or [i for i in range(1, amount) if given[i] < most]
        whole, left = sum([weights[i] for i in movable]), surplus
        for i in movable:
            more = min(most - given[i], max(1, left * weights[i] // whole), surplus)
            given[i] = given[i] + more
            surplus = surplus - more
    return np.array(given)


def normal_values(key, shape, scale, bound, split=(), kind=jnp.bfloat16):
    factor_of = block_levels(key, shape, split, -0.22, 0.18) if split else 1.0
    drawn = jax.random.normal(key, shape, jnp.float32) * scale * factor_of
    return jnp.minimum(jnp.maximum(drawn, -bound), bound).astype(kind)


def setup_inputs(seed: int = 0) -> dict:
    streams_of = jax.random.split(jax.random.key(seed), 13)
    queries = draw_queries(jax.random.fold_in(streams_of[12], 71), 0)
    keys = draw_keys(jax.random.fold_in(streams_of[12], 71), 0)
    values = draw_values(jax.random.fold_in(streams_of[12], 71), 0)
    residual = draw_residual(jax.random.fold_in(streams_of[12], 71), 0)
    proj_weight = normal_values(streams_of[4], (HEADS * HEAD_DIM, D), (HEADS * HEAD_DIM) ** -0.5, 0.109375, ((0, 4), (1, 8)))
    norm_gain = jnp.clip(1.0 + 0.18 * jax.random.normal(streams_of[5], (D,), jnp.float32), 0.099609375, 1.8984375).astype(jnp.bfloat16)
    router = normal_values(streams_of[6], (D, EXPERTS), D ** -0.5, 0.078125)
    expert_ids_keys = jax.random.split(jax.random.fold_in(streams_of[7], 1), TOKENS // TOK_DEV)
    expert_ids_turns = jax.random.permutation(jax.random.fold_in(streams_of[7], 3), TOKENS // TOK_DEV)
    expert_ids = jax.vmap(lambda own, number: assign_block(jax.random.fold_in(streams_of[7], 2), own, number, TOK_DEV, EXPERTS, TOP, CAP, 2))(expert_ids_keys, expert_ids_turns).reshape((TOKENS, TOP))
    u_gate_up = normal_values(streams_of[8], (EXPERTS * PIECES, D // PIECES, 2 * RANK), D ** -0.5, 0.078125, ((0, 8),))
    v_gate_up = normal_values(streams_of[9], (EXPERTS * PIECES, 2, RANK, FF // PIECES), RANK ** -0.5, 0.25, ((0, 8),))
    u_down = normal_values(streams_of[10], (EXPERTS * PIECES, FF // PIECES, RANK), FF ** -0.5, 0.0625, ((0, 8),))
    v_down = normal_values(streams_of[11], (EXPERTS * PIECES, RANK, D // PIECES), RANK ** -0.5, 0.25, ((0, 8),))
    return {"queries": queries, "keys": keys, "values": values, "residual": residual, "proj_weight": proj_weight, "norm_gain": norm_gain, "router": router, "expert_ids": expert_ids, "u_gate_up": u_gate_up, "v_gate_up": v_gate_up, "u_down": u_down, "v_down": v_down}


EPS = 1e-05

def causal_attention(queries, keys, values):
    tile_rows = min(1024, TOKENS)
    tile_count = TOKENS // tile_rows
    per_kv = HEADS // KV_HEADS
    query_tiles = queries.reshape(tile_count, tile_rows, KV_HEADS, per_kv, HEAD_DIM)
    key_tiles = keys.reshape(tile_count, tile_rows, KV_HEADS, HEAD_DIM)
    value_tiles = values.reshape(tile_count, tile_rows, KV_HEADS, HEAD_DIM)
    score_scale = HEAD_DIM ** (-0.5)
    offsets = jnp.arange(tile_rows, dtype=jnp.int32)

    def one_tile(tile_index):
        query_block = lax.dynamic_index_in_dim(query_tiles, tile_index, 0, keepdims=False).astype(jnp.float32)
        query_pos = tile_index * tile_rows + offsets

        def scores_of(key_index):
            key_block = lax.dynamic_index_in_dim(key_tiles, key_index, 0, keepdims=False).astype(jnp.float32)
            scores = jnp.einsum('qhjd,khd->hjqk', query_block, key_block) * score_scale
            key_pos = key_index * tile_rows + offsets
            allowed = key_pos[None, :] <= query_pos[:, None]
            return jnp.where(allowed[None, None], scores, -jnp.inf)

        def max_step(key_index, row_max):
            return jnp.maximum(row_max, lax.optimization_barrier(jnp.max(scores_of(key_index), axis=-1)))
        start_max = jnp.full((KV_HEADS, per_kv, tile_rows), -jnp.inf, jnp.float32)
        row_max = lax.fori_loop(jnp.int32(0), tile_index + 1, max_step, start_max)

        def sum_step(key_index, carried):
            row_sum, weighted = carried
            exp_terms = jnp.exp(scores_of(key_index) - row_max[..., None])
            rounded = lax.optimization_barrier(exp_terms.astype(jnp.bfloat16)).astype(jnp.float32)
            value_block = lax.dynamic_index_in_dim(value_tiles, key_index, 0, keepdims=False).astype(jnp.float32)
            row_sum = row_sum + lax.optimization_barrier(jnp.sum(exp_terms, axis=-1))
            weighted = weighted + jnp.einsum('hjqk,khd->hjqd', rounded, value_block)
            return (row_sum, weighted)
        start_sum = jnp.zeros((KV_HEADS, per_kv, tile_rows), jnp.float32)
        start_acc = jnp.zeros((KV_HEADS, per_kv, tile_rows, HEAD_DIM), jnp.float32)
        row_sum, weighted = lax.fori_loop(jnp.int32(0), tile_index + 1, sum_step, (start_sum, start_acc))
        result = weighted / row_sum[..., None]
        return jnp.transpose(result, (2, 0, 1, 3)).reshape(tile_rows, HEADS * HEAD_DIM)
    outputs = lax.map(one_tile, jnp.arange(tile_count, dtype=jnp.int32))
    return outputs.reshape(TOKENS, HEADS * HEAD_DIM).astype(jnp.bfloat16)

def expert_stack(u_gate_up, v_gate_up, u_down, v_down):
    first_in = u_gate_up.reshape(EXPERTS, D, 2 * RANK)
    second_in = jnp.transpose(v_gate_up.reshape(EXPERTS, PIECES, 2, RANK, FF // PIECES), (0, 2, 3, 1, 4))
    second_in = second_in.reshape(EXPERTS, 2, RANK, FF)
    first_out = u_down.reshape(EXPERTS, FF, RANK)
    second_out = jnp.transpose(v_down.reshape(EXPERTS, PIECES, RANK, D // PIECES), (0, 2, 1, 3))
    second_out = second_out.reshape(EXPERTS, RANK, D)
    return (first_in, second_in, first_out, second_out)

def reference(queries, keys, values, residual, proj_weight, norm_gain, router, expert_ids, u_gate_up, v_gate_up, u_down, v_down):
    attended = causal_attention(queries, keys, values)
    attn_update = jnp.dot(attended, proj_weight, preferred_element_type=jnp.float32).astype(jnp.bfloat16)
    stream = residual.astype(jnp.float32) + attn_update.astype(jnp.float32)
    mean_sq = lax.optimization_barrier(jnp.mean(stream * stream, axis=-1, keepdims=True))
    normed = (stream * lax.rsqrt(mean_sq + EPS) * norm_gain.astype(jnp.float32)).astype(jnp.bfloat16)
    logits = jnp.dot(normed, router, preferred_element_type=jnp.float32)
    expert_range = jnp.arange(EXPERTS, dtype=jnp.int32)
    picked = (expert_ids[:, :, None] == expert_range[None, None, :]).astype(jnp.float32)
    chosen = lax.optimization_barrier(jnp.sum(picked * logits[:, None, :], axis=-1))
    mix_first = jax.nn.sigmoid(chosen[:, 0] - chosen[:, 1])
    mix_second = jax.nn.sigmoid(chosen[:, 1] - chosen[:, 0])
    mix_weight = jnp.stack([mix_first, mix_second], axis=1)
    block_count = TOKENS // TOK_DEV
    normed_blocks = normed.reshape(block_count, TOK_DEV, D).astype(jnp.float32)
    ids_blocks = expert_ids.reshape(block_count, TOK_DEV * 2)
    weight_blocks = mix_weight.reshape(block_count, TOK_DEV, 2)
    slot_range = jnp.arange(CAP, dtype=jnp.int32)
    first_in, second_in, first_out, second_out = expert_stack(u_gate_up, v_gate_up, u_down, v_down)

    def one_expert(carried, expert_index):
        member = (ids_blocks == expert_index).astype(jnp.int32)
        slot_of = jnp.cumsum(member, axis=1) - 1
        placed = (member[..., None] * (slot_of[..., None] == slot_range).astype(jnp.int32)).astype(jnp.float32)
        placed_tok = placed.reshape(block_count, TOK_DEV, 2, CAP)
        select = lax.optimization_barrier(jnp.sum(placed_tok, axis=2))
        rows_in = jnp.einsum('btc,btd->bcd', select, normed_blocks).astype(jnp.bfloat16)
        rows_in = rows_in.reshape(block_count * CAP, D)
        w_first = lax.dynamic_index_in_dim(first_in, expert_index, 0, keepdims=False)
        w_middle = lax.dynamic_index_in_dim(second_in, expert_index, 0, keepdims=False)
        w_down = lax.dynamic_index_in_dim(first_out, expert_index, 0, keepdims=False)
        w_last = lax.dynamic_index_in_dim(second_out, expert_index, 0, keepdims=False)
        rank_in = jnp.dot(rows_in, w_first, preferred_element_type=jnp.float32).astype(jnp.bfloat16)
        gate_part = jnp.dot(rank_in[:, :RANK], w_middle[0], preferred_element_type=jnp.float32)
        up_part = jnp.dot(rank_in[:, RANK:], w_middle[1], preferred_element_type=jnp.float32)
        hidden = (jax.nn.silu(gate_part) * up_part).astype(jnp.bfloat16)
        rank_down = jnp.dot(hidden, w_down, preferred_element_type=jnp.float32).astype(jnp.bfloat16)
        out_rows = jnp.dot(rank_down, w_last, preferred_element_type=jnp.float32).astype(jnp.bfloat16)
        back_rows = out_rows.astype(jnp.float32).reshape(block_count, CAP, D)
        weights_tok = jnp.einsum('btsc,bts->btc', placed_tok, weight_blocks)
        carried = carried + jnp.einsum('btc,bcd->btd', weights_tok, back_rows)
        return (carried, None)
    start_mix = jnp.zeros((block_count, TOK_DEV, D), jnp.float32)
    mixture, unused = lax.scan(one_expert, start_mix, jnp.arange(EXPERTS, dtype=jnp.int32))
    return (stream + mixture.reshape(TOKENS, D)).astype(jnp.bfloat16)
```

```python
import functools

import jax
import jax.numpy as jnp
from jax import lax
from jax.experimental import pallas as pl
from jax.experimental.pallas import tpu as pltpu
from jax.sharding import PartitionSpec as P

D = 6144
HEADS = 24
KV_HEADS = 4
HEAD_DIM = 128
EXPERTS = 8
RANK = 512
TOK_DEV = 128
CAP = 33


EPS = 1e-05
LOG2_E = 1.4426950408889634


def attention_kernel(heads, parts, q_ref, kv_ref, out_ref):
    block = pl.program_id(0)
    column = lax.axis_index("exp")
    columns = kv_ref.shape[0]
    span = columns // parts
    chunk = span * TOK_DEV
    rows = heads * TOK_DEV
    query = jnp.concatenate(
        [q_ref[:, h * HEAD_DIM : (h + 1) * HEAD_DIM] for h in range(heads)], axis=0
    )

    def step(index, carried, masked):
        row_max, row_sum, weighted = carried
        held = kv_ref[pl.ds((index % parts) * span, span), index // parts]
        held = held.reshape(chunk, 2 * HEAD_DIM)
        scores = lax.dot_general(
            query, held[:, :HEAD_DIM], (((1,), (1,)), ((), ())), preferred_element_type=jnp.float32
        ) * (HEAD_DIM ** (-0.5) * LOG2_E)
        if masked:
            offset = (column % span) * TOK_DEV
            own = lax.broadcasted_iota(jnp.int32, (rows, chunk), 0) % TOK_DEV + offset
            other = lax.broadcasted_iota(jnp.int32, (rows, chunk), 1)
            scores = jnp.where(other <= own, scores, -jnp.inf)
        new_max = jnp.maximum(row_max, jnp.max(scores, axis=-1, keepdims=True))
        fading = jnp.exp2(row_max - new_max)
        terms = jnp.exp2(scores - new_max)
        row_sum = row_sum * fading + jnp.sum(terms, axis=-1, keepdims=True)
        update = jnp.dot(
            terms.astype(jnp.bfloat16), held[:, HEAD_DIM:], preferred_element_type=jnp.float32
        )
        return new_max, row_sum, weighted * fading + update

    carried = (
        jnp.full((rows, 1), -1e30, jnp.float32),
        jnp.zeros((rows, 1), jnp.float32),
        jnp.zeros((rows, HEAD_DIM), jnp.float32),
    )
    last = block * parts + column // span
    carried = lax.fori_loop(0, last, lambda index, now: step(index, now, False), carried)
    row_max, row_sum, weighted = step(last, carried, True)
    result = (weighted / row_sum).astype(jnp.bfloat16)
    for h in range(heads):
        out_ref[:, h * HEAD_DIM : (h + 1) * HEAD_DIM] = result[h * TOK_DEV : (h + 1) * TOK_DEV]


def attention(query_rows, kv_all, heads):
    columns, blocks = kv_all.shape[:2]
    parts = max(1, columns * TOK_DEV // 512)
    width = heads * HEAD_DIM
    pairs = blocks * TOK_DEV * heads * columns * blocks * TOK_DEV // 2
    return pl.pallas_call(
        functools.partial(attention_kernel, heads, parts),
        grid=(blocks,),
        out_shape=jax.ShapeDtypeStruct((blocks * TOK_DEV, width), jnp.bfloat16),
        in_specs=[
            pl.BlockSpec((TOK_DEV, width), lambda b: (b, 0)),
            pl.BlockSpec(kv_all.shape, lambda b: (0, 0, 0, 0)),
        ],
        out_specs=pl.BlockSpec((TOK_DEV, width), lambda b: (b, 0)),
        compiler_params=pltpu.CompilerParams(vmem_limit_bytes=56 * 1024 * 1024),
        cost_estimate=pl.CostEstimate(
            flops=pairs * 4 * HEAD_DIM * 4,
            bytes_accessed=kv_all.size * 2,
            transcendentals=pairs,
        ),
        name="attention",
    )(query_rows, kv_all)


MAIN = CAP // 16 * 16
PAD = 16


def flipped(index, bits):
    bit = 1
    while bit <= bits:
        if bits & bit:
            index = index + bit * (1 - 2 * ((index // bit) % 2))
        bit *= 2
    return index


def to_exp(peer):
    return {"device_id": {"exp": peer}, "device_id_type": pl.DeviceIdType.MESH}


def gather_lanes(ref, chunk, tiles):
    return jnp.concatenate([ref[chunk, :, t, :] for t in range(tiles)], axis=1)


def padded(rows):
    count = rows.shape[0]
    if count % PAD:
        rows = jnp.concatenate(
            [rows, jnp.zeros((PAD - count % PAD, rows.shape[1]), rows.dtype)], axis=0
        )
    return rows.astype(jnp.bfloat16)


def experts_kernel(
    count,
    pieces,
    chunks,
    steps,
    x_ref,
    sel_ref,
    mix_ref,
    stream_ref,
    u_hbm,
    vg_hbm,
    ud_hbm,
    vd_hbm,
    out_ref,
    u_buf,
    vg_buf,
    ud_buf,
    vd_buf,
    send,
    recv,
    back,
    send_x,
    recv_x,
    back_x,
    rank_sum,
    rank_in,
    swap,
    w_sem,
    send_sem,
    recv_sem,
    send_x_sem,
    recv_x_sem,
    swap_sem,
):
    me = lax.axis_index("exp")
    experts = count // pieces
    width = send.shape[-1]
    tiles = width // 128
    unit = vg_buf.shape[-1]
    barrier = pltpu.get_barrier_semaphore()
    for d in range(1, count):
        pl.semaphore_signal(barrier, inc=1, **to_exp(flipped(me, d)))

    def u_copy(c):
        rows = pl.ds(pl.multiple_of(c * width, width), width)
        return pltpu.make_async_copy(u_hbm.at[0, rows], u_buf.at[c], w_sem.at[0, c])

    def vg_copy(f):
        cols = pl.ds(pl.multiple_of(f * unit, unit), unit)
        return pltpu.make_async_copy(vg_hbm.at[0, :, :, cols], vg_buf.at[f], w_sem.at[1, f])

    def ud_copy(f):
        rows = pl.ds(pl.multiple_of(f * unit, unit), unit)
        return pltpu.make_async_copy(ud_hbm.at[0, rows], ud_buf.at[f], w_sem.at[2, f])

    def vd_copy(c):
        cols = pl.ds(pl.multiple_of(c * width, width), width)
        return pltpu.make_async_copy(vd_hbm.at[0, :, cols], vd_buf.at[c], w_sem.at[3, c])

    for c in range(chunks):
        u_copy(c).start()
    for f in range(steps):
        vg_copy(f).start()
        ud_copy(f).start()
    for c in range(chunks):
        vd_copy(c).start()

    def fill(c, piece, rows):
        for k in range(experts):
            send[c, k * pieces + piece] = rows[k * MAIN : (k + 1) * MAIN].astype(jnp.bfloat16)
        extra = rows[experts * MAIN : experts * MAIN + experts]
        for t in range(tiles):
            lanes = extra[:, t * 128 : (t + 1) * 128]
            if pieces == 1:
                send_x[c, :, t, :] = lanes
            else:
                for k in range(experts):
                    send_x[c, k * pieces + piece, t : t + 1, :] = lanes[k : k + 1]

    def copies(phase, c, peer, into, into_x):
        main = pltpu.make_async_remote_copy(
            src_ref=send.at[c, peer],
            dst_ref=into.at[c, me],
            send_sem=send_sem.at[phase, c, peer],
            recv_sem=recv_sem.at[phase, c, me],
            **to_exp(peer),
        )
        extra = pltpu.make_async_remote_copy(
            src_ref=send_x.at[c, peer],
            dst_ref=into_x.at[c, me],
            send_sem=send_x_sem.at[phase, c, peer],
            recv_sem=recv_x_sem.at[phase, c, me],
            **to_exp(peer),
        )
        return main, extra

    def arrivals(phase, c, peer, into, into_x):
        main = pltpu.make_async_remote_copy(
            src_ref=send.at[c, peer],
            dst_ref=into.at[c, peer],
            send_sem=send_sem.at[phase, c, peer],
            recv_sem=recv_sem.at[phase, c, peer],
            **to_exp(peer),
        )
        extra = pltpu.make_async_remote_copy(
            src_ref=send_x.at[c, peer],
            dst_ref=into_x.at[c, peer],
            send_sem=send_x_sem.at[phase, c, peer],
            recv_sem=recv_x_sem.at[phase, c, peer],
            **to_exp(peer),
        )
        return main, extra

    def send_all(phase, c, into, into_x):
        for d in range(1, count):
            for copy in copies(phase, c, flipped(me, d), into, into_x):
                copy.start()
        into[c, me] = send[c, me]
        into_x[c, me] = send_x[c, me]

    def wait_sent(phase, c, into, into_x):
        for d in range(1, count):
            for copy in arrivals(phase, c, flipped(me, d), into, into_x):
                copy.wait_send()

    def wait_got(phase, c, into, into_x):
        for d in range(1, count):
            for copy in arrivals(phase, c, flipped(me, d), into, into_x):
                copy.wait_recv()

    def fill_first(c):
        for piece in range(pieces):
            start = pl.multiple_of(piece * chunks * width + c * width, width)
            fill(
                c,
                piece,
                jnp.dot(
                    sel_ref[...],
                    x_ref[:, pl.ds(start, width)],
                    preferred_element_type=jnp.float32,
                ),
            )

    fill_first(0)
    pl.semaphore_wait(barrier, count - 1)
    send_all(0, 0, recv, recv_x)

    def dispatch(c, carried):
        fill_first(c)
        send_all(0, c, recv, recv_x)
        return carried

    lax.fori_loop(1, chunks, dispatch, 0)
    rank_sum[...] = jnp.zeros_like(rank_sum)

    def first_factor(c, carried):
        u_copy(c).wait()
        wait_got(0, c, recv, recv_x)
        rows = jnp.concatenate(
            [recv[c].reshape(count * MAIN, width), padded(gather_lanes(recv_x, c, tiles))], axis=0
        )
        rank_sum[...] += jnp.dot(rows, u_buf[c], preferred_element_type=jnp.float32)
        return carried

    lax.fori_loop(0, chunks, first_factor, 0)

    def add_pieces(slot, columns):
        bit = 1
        while bit < pieces:
            swap[slot, 0, :, :columns] = rank_sum[:, :columns].astype(jnp.bfloat16)
            copy = pltpu.make_async_remote_copy(
                src_ref=swap.at[slot, 0],
                dst_ref=swap.at[slot, 1],
                send_sem=swap_sem.at[slot, 0],
                recv_sem=swap_sem.at[slot, 1],
                **to_exp(flipped(me, bit)),
            )
            copy.start()
            copy.wait()
            rank_sum[:, :columns] += swap[slot, 1, :, :columns].astype(jnp.float32)
            bit *= 2
            slot += 1
        return slot

    slot = add_pieces(0, 2 * RANK)
    rank_in[...] = rank_sum[...].astype(jnp.bfloat16)
    rank_sum[:, :RANK] = jnp.zeros((rank_sum.shape[0], RANK), jnp.float32)

    def middle(f, carried):
        vg_copy(f).wait()
        ud_copy(f).wait()
        gate = jnp.dot(rank_in[:, :RANK], vg_buf[f, 0], preferred_element_type=jnp.float32)
        up = jnp.dot(rank_in[:, RANK:], vg_buf[f, 1], preferred_element_type=jnp.float32)
        hidden = (gate / (1.0 + jnp.exp(-gate)) * up).astype(jnp.bfloat16)
        rank_sum[:, :RANK] += jnp.dot(hidden, ud_buf[f], preferred_element_type=jnp.float32)
        return carried

    lax.fori_loop(0, steps, middle, 0)
    add_pieces(slot, RANK)
    rank_in[:, :RANK] = rank_sum[:, :RANK].astype(jnp.bfloat16)

    def last_factor(c, carried):
        vd_copy(c).wait()
        wait_sent(0, c, recv, recv_x)
        rows = jnp.dot(rank_in[:, :RANK], vd_buf[c], preferred_element_type=jnp.float32)
        for k in range(count):
            send[c, k] = rows[k * MAIN : (k + 1) * MAIN].astype(jnp.bfloat16)
        extra = rows[count * MAIN : count * MAIN + count]
        for t in range(tiles):
            send_x[c, :, t, :] = extra[:, t * 128 : (t + 1) * 128]
        send_all(1, c, back, back_x)
        return carried

    lax.fori_loop(0, chunks, last_factor, 0)

    def combine(c, carried):
        wait_got(1, c, back, back_x)
        for piece in range(pieces):
            rows = back[c].reshape(experts, pieces, MAIN, width)[:, piece]
            extra = gather_lanes(back_x, c, tiles).reshape(experts, pieces, width)[:, piece]
            rows = jnp.concatenate([rows.reshape(experts * MAIN, width), padded(extra)], axis=0)
            both = jnp.dot(mix_ref[...], rows, preferred_element_type=jnp.float32)
            start = pl.multiple_of(piece * chunks * width + c * width, width)
            cols = pl.ds(start, width)
            out_ref[:, cols] = (
                stream_ref[:, cols] + both[:TOK_DEV] + both[TOK_DEV:]
            ).astype(jnp.bfloat16)
        return carried

    lax.fori_loop(0, chunks, combine, 0)

    def drain(c, carried):
        wait_sent(1, c, back, back_x)
        return carried

    lax.fori_loop(0, chunks, drain, 0)


def experts_layer(normed, select, mix, stream, u_gate_up, v_gate_up, u_down, v_down, chunks):
    count = lax.axis_size("exp")
    pieces = count // EXPERTS
    width = D // pieces // chunks
    units = u_down.shape[1]
    unit = min(1024, units)
    steps = units // unit
    rows = count * MAIN + PAD * (-(-count // PAD))
    swaps = max(1, 2 * (pieces.bit_length() - 1))
    vmem = pl.BlockSpec(memory_space=pltpu.VMEM)
    anywhere = pl.BlockSpec(memory_space=pl.ANY)
    dma = pltpu.SemaphoreType.DMA
    block = (chunks, count, MAIN, width)
    block_x = (chunks, count, width // 128, 128)
    return pl.pallas_call(
        functools.partial(experts_kernel, count, pieces, chunks, steps),
        out_shape=jax.ShapeDtypeStruct((TOK_DEV, D), jnp.bfloat16),
        in_specs=[vmem] * 4 + [anywhere] * 4,
        out_specs=vmem,
        scratch_shapes=[
            pltpu.VMEM((chunks, width, 2 * RANK), jnp.bfloat16),
            pltpu.VMEM((steps, 2, RANK, unit), jnp.bfloat16),
            pltpu.VMEM((steps, unit, RANK), jnp.bfloat16),
            pltpu.VMEM((chunks, RANK, width), jnp.bfloat16),
            pltpu.VMEM(block, jnp.bfloat16),
            pltpu.VMEM(block, jnp.bfloat16),
            pltpu.VMEM(block, jnp.bfloat16),
            pltpu.VMEM(block_x, jnp.float32),
            pltpu.VMEM(block_x, jnp.float32),
            pltpu.VMEM(block_x, jnp.float32),
            pltpu.VMEM((rows, 2 * RANK), jnp.float32),
            pltpu.VMEM((rows, 2 * RANK), jnp.bfloat16),
            pltpu.VMEM((swaps, 2, rows, 2 * RANK) if pieces > 1 else (1, 2, 16, 128), jnp.bfloat16),
            dma((4, max(chunks, steps))),
            dma((2, chunks, count)),
            dma((2, chunks, count)),
            dma((2, chunks, count)),
            dma((2, chunks, count)),
            dma((swaps, 2)),
        ],
        compiler_params=pltpu.CompilerParams(
            collective_id=0, has_side_effects=True, vmem_limit_bytes=67043328
        ),
        cost_estimate=pl.CostEstimate(
            flops=rows * RANK * units * 6,
            bytes_accessed=units * RANK * 6,
            transcendentals=rows * units,
        ),
        name="experts",
    )(normed, select, mix, stream, u_gate_up, v_gate_up, u_down, v_down)


def per_device(
    queries,
    keys,
    values,
    residual,
    proj_weight,
    norm_gain,
    router,
    expert_ids,
    u_gate_up,
    v_gate_up,
    u_down,
    v_down,
):
    seq_count = lax.axis_size("seq")
    exp_count = lax.axis_size("exp")
    heads = HEADS // seq_count
    shares = seq_count // KV_HEADS
    kv_send = jnp.concatenate(
        [keys.reshape(TOK_DEV, KV_HEADS, HEAD_DIM), values.reshape(TOK_DEV, KV_HEADS, HEAD_DIM)],
        axis=-1,
    )
    if shares > 1:
        kv_send = jnp.repeat(kv_send, shares, axis=1)
    kv_send = kv_send.reshape(TOK_DEV, seq_count * 2 * HEAD_DIM)
    kv_got = lax.all_to_all(kv_send, "seq", split_axis=1, concat_axis=0, tiled=True)
    kv_all = lax.all_gather(kv_got, "exp", axis=0, tiled=False)
    query_got = lax.all_to_all(queries, "seq", split_axis=1, concat_axis=0, tiled=True)
    query_got, weight_own = lax.optimization_barrier((query_got, proj_weight))
    weight_rows = lax.all_gather(weight_own, "seq", axis=0, tiled=True)
    kv_all = kv_all.reshape(exp_count, seq_count, TOK_DEV, 2 * HEAD_DIM)
    attended = attention(query_got, kv_all, heads)
    attended = lax.all_to_all(attended, "seq", split_axis=0, concat_axis=1, tiled=True)
    half = TOK_DEV // 2
    first_half, weight_rows = lax.optimization_barrier((attended[:half], weight_rows))
    gathered = [
        lax.all_gather(first_half, "exp", axis=0, tiled=True),
        lax.all_gather(attended[half:], "exp", axis=0, tiled=True),
    ]
    updates = []
    for rows in gathered:
        projected = jnp.dot(rows, weight_rows, preferred_element_type=jnp.float32)
        updates.append(
            lax.all_to_all(
                projected.astype(jnp.bfloat16), "exp", split_axis=0, concat_axis=1, tiled=True
            )
        )
    attn_update = jnp.concatenate(updates, axis=0)
    stream = residual.astype(jnp.float32) + attn_update.astype(jnp.float32)
    mean_sq = jnp.mean(stream * stream, axis=-1, keepdims=True)
    normed = (stream * lax.rsqrt(mean_sq + EPS) * norm_gain.astype(jnp.float32)).astype(
        jnp.bfloat16
    )
    logits = jnp.dot(normed, router, preferred_element_type=jnp.float32)
    expert_range = jnp.arange(EXPERTS, dtype=jnp.int32)
    picked = (expert_ids[:, :, None] == expert_range[None, None, :]).astype(jnp.float32)
    chosen = jnp.sum(picked * logits[:, None, :], axis=-1)
    mix_first = jax.nn.sigmoid(chosen[:, 0] - chosen[:, 1])
    mix_second = jax.nn.sigmoid(chosen[:, 1] - chosen[:, 0])
    flat_ids = expert_ids.reshape(TOK_DEV * 2)
    member = (flat_ids[:, None] == expert_range[None, :]).astype(jnp.int32)
    slot_of = jnp.sum((jnp.cumsum(member, axis=0) - 1) * member, axis=1)
    dest = jnp.where(
        slot_of < MAIN, flat_ids * MAIN + slot_of, EXPERTS * MAIN + flat_ids + (slot_of - MAIN)
    ).reshape(TOK_DEV, 2)
    places = jnp.arange(EXPERTS * MAIN + PAD, dtype=jnp.int32)
    first_at = dest[:, 0:1] == places[None, :]
    second_at = dest[:, 1:2] == places[None, :]
    select = (
        (dest[:, 0][None, :] == places[:, None]) | (dest[:, 1][None, :] == places[:, None])
    ).astype(jnp.bfloat16)
    mix = mix_first[:, None] * first_at.astype(jnp.float32) + mix_second[
        :, None
    ] * second_at.astype(jnp.float32)
    mix_high = lax.reduce_precision(mix, 8, 7)
    mix_low = (mix - mix_high).astype(jnp.bfloat16)
    mix_both = jnp.concatenate([mix_high.astype(jnp.bfloat16), mix_low], axis=0)
    return experts_layer(
        normed, select, mix_both, stream, u_gate_up, v_gate_up, u_down, v_down, 3
    )


def solution(mesh):
    in_specs = (
        P(("seq", "exp"), None),
        P(("seq", "exp"), None),
        P(("seq", "exp"), None),
        P(("seq", "exp"), None),
        P("seq", "exp"),
        P(),
        P(),
        P(("seq", "exp"), None),
        P("exp", None, None),
        P("exp", None, None, None),
        P("exp", None, None),
        P("exp", None, None),
    )
    out_specs = P(("seq", "exp"), None)
    return jax.shard_map(
        per_device, mesh=mesh, in_specs=in_specs, out_specs=out_specs, check_vma=False
    )
```

```python
import functools

import jax
import jax.numpy as jnp
from jax import lax
from jax.experimental import pallas as pl
from jax.experimental.pallas import tpu as pltpu
from jax.sharding import PartitionSpec as P

D = 6144
HEADS = 24
KV_HEADS = 4
HEAD_DIM = 128
EXPERTS = 8
RANK = 512
TOK_DEV = 128
CAP = 33


EPS = 1e-05
LOG2_E = 1.4426950408889634


MAIN = CAP // 16 * 16
PAD = 16
PIECE = 384
AHEAD = 3


def flipped(index, bits):
    bit = 1
    while bit <= bits:
        if bits & bit:
            index = index + bit * (1 - 2 * ((index // bit) % 2))
        bit *= 2
    return index


def at(**place):
    return {"device_id": place, "device_id_type": pl.DeviceIdType.MESH}


def greet(seq_count, exp_count):
    seq, exp = lax.axis_index("seq"), lax.axis_index("exp")
    barrier = pltpu.get_barrier_semaphore()
    for d in range(1, exp_count):
        pl.semaphore_signal(barrier, inc=1, **at(exp=flipped(exp, d)))
    for d in range(1, seq_count):
        for c in range(2):
            pl.semaphore_signal(
                barrier, inc=1, **at(seq=flipped(seq, d), exp=flipped(exp, c))
            )
    return barrier, exp_count - 1 + 2 * (seq_count - 1)


MAIN = CAP // 16 * 16
PAD = 16
PIECE = 384
AHEAD = 3


def flipped(index, bits):
    bit = 1
    while bit <= bits:
        if bits & bit:
            index = index + bit * (1 - 2 * ((index // bit) % 2))
        bit *= 2
    return index


def at(**place):
    return {"device_id": place, "device_id_type": pl.DeviceIdType.MESH}


def greet(seq_count, exp_count):
    seq, exp = lax.axis_index("seq"), lax.axis_index("exp")
    barrier = pltpu.get_barrier_semaphore()
    for d in range(1, exp_count):
        pl.semaphore_signal(barrier, inc=1, **at(exp=flipped(exp, d)))
    for d in range(1, seq_count):
        for c in range(2):
            pl.semaphore_signal(
                barrier, inc=1, **at(seq=flipped(seq, d), exp=flipped(exp, c))
            )
    return barrier, exp_count - 1 + 2 * (seq_count - 1)


def attention_kernel(
    seq_count,
    exp_count,
    q_ref,
    k_ref,
    v_ref,
    w_hbm,
    out_ref,
    near_hbm,
    q_all,
    kv_all,
    in_send,
    in_recv,
    q_send,
    q_recv,
    kv_send,
    kv_recv,
    w_send,
    w_recv,
    out_send,
    out_recv,
):
    seq, exp = lax.axis_index("seq"), lax.axis_index("exp")
    chips = exp_count // 2
    chip, core = exp // 2, exp % 2
    heads = HEADS // seq_count
    width = heads * HEAD_DIM
    shares = max(1, seq_count // KV_HEADS)
    barrier, greetings = greet(seq_count, exp_count)
    own = pl.ds(pl.multiple_of((seq // shares) * HEAD_DIM, HEAD_DIM), HEAD_DIM)
    kv_all[exp, seq, :, :HEAD_DIM] = k_ref[:, own]
    kv_all[exp, seq, :, HEAD_DIM:] = v_ref[:, own]
    q_all[seq] = q_ref[:, pl.ds(pl.multiple_of(seq * width, width), width)]
    pl.semaphore_wait(barrier, greetings)

    def kv_copy(half, peer, block):
        ref = (k_ref, v_ref)[half]
        head = pl.ds(pl.multiple_of((peer // shares) * HEAD_DIM, HEAD_DIM), HEAD_DIM)
        return pltpu.make_async_remote_copy(
            src_ref=ref.at[:, head],
            dst_ref=kv_all.at[exp, block, :, pl.ds(half * HEAD_DIM, HEAD_DIM)],
            send_sem=in_send.at[half, peer],
            recv_sem=in_recv.at[half, block],
            **at(seq=peer),
        )

    def q_copy(peer, block):
        return pltpu.make_async_remote_copy(
            src_ref=q_ref.at[:, pl.ds(pl.multiple_of(peer * width, width), width)],
            dst_ref=q_all.at[block],
            send_sem=q_send.at[peer],
            recv_sem=q_recv.at[block],
            **at(seq=peer),
        )

    for d in range(1, seq_count):
        for half in range(2):
            kv_copy(half, flipped(seq, d), seq).start()
    for d in range(1, seq_count):
        q_copy(flipped(seq, d), seq).start()

    def pass_on(way, block, target):
        return pltpu.make_async_remote_copy(
            src_ref=kv_all.at[block],
            dst_ref=kv_all.at[block],
            send_sem=kv_send.at[way, block],
            recv_sem=kv_recv.at[block],
            **at(exp=target),
        )

    def weight(way, target):
        return pltpu.make_async_remote_copy(
            src_ref=w_hbm,
            dst_ref=near_hbm.at[way],
            send_sem=w_send.at[way],
            recv_sem=w_recv.at[way],
            **at(exp=target),
        )

    partner = flipped(exp, 1)

    def spread(block, up, down, act):
        if up:

            @pl.when(chip + 1 < chips)
            def _():
                act(pass_on(0, block, exp + 2))

        if down:

            @pl.when(chip >= 1)
            def _():
                act(pass_on(1, block, exp - 2))

        act(pass_on(2, block, partner))

    def start(copy):
        copy.start()

    def sent(copy):
        copy.wait_send()

    for d in range(1, seq_count):
        for half in range(2):
            peer = flipped(seq, d)
            kv_copy(half, peer, peer).wait_recv()
    spread(exp, True, True, start)

    def relay(act, wait):
        for hop in range(1, chips):
            below, above = exp - 2 * hop, exp + 2 * hop

            @pl.when(chip >= hop)
            def _():
                if wait:
                    pass_on(2, below, partner).wait_recv()
                spread(below, True, False, act)

            @pl.when(chip + hop < chips)
            def _():
                if wait:
                    pass_on(2, above, partner).wait_recv()
                spread(above, False, True, act)

    relay(start, True)

    @pl.when(chip + 1 < chips)
    def _():
        weight(0, exp + 2).start()

    @pl.when(chip >= 1)
    def _():
        weight(1, exp - 2).start()

    for other in range(chips):
        pass_on(2, 2 * other + 1 - core, partner).wait_recv()
    for d in range(1, seq_count):
        peer = flipped(seq, d)
        q_copy(peer, peer).wait_recv()

    parts = max(1, exp_count * TOK_DEV // 512)
    span = exp_count // parts
    chunk = span * TOK_DEV
    rows = heads * TOK_DEV

    def attend(block, unused):
        query = jnp.concatenate(
            [q_all[block, :, h * HEAD_DIM : (h + 1) * HEAD_DIM] for h in range(heads)], axis=0
        )

        def step(index, carried, masked):
            row_max, row_sum, weighted = carried
            held = kv_all[pl.ds((index % parts) * span, span), index // parts]
            held = held.reshape(chunk, 2 * HEAD_DIM)
            scores = lax.dot_general(
                query,
                held[:, :HEAD_DIM],
                (((1,), (1,)), ((), ())),
                preferred_element_type=jnp.float32,
            ) * (HEAD_DIM ** (-0.5) * LOG2_E)
            if masked:
                offset = (exp % span) * TOK_DEV
                mine = lax.broadcasted_iota(jnp.int32, (rows, chunk), 0) % TOK_DEV + offset
                other = lax.broadcasted_iota(jnp.int32, (rows, chunk), 1)
                scores = jnp.where(other <= mine, scores, -jnp.inf)
            new_max = jnp.maximum(row_max, jnp.max(scores, axis=-1, keepdims=True))
            fading = jnp.exp2(row_max - new_max)
            terms = jnp.exp2(scores - new_max)
            row_sum = row_sum * fading + jnp.sum(terms, axis=-1, keepdims=True)
            update = jnp.dot(
                terms.astype(jnp.bfloat16), held[:, HEAD_DIM:], preferred_element_type=jnp.float32
            )
            return new_max, row_sum, weighted * fading + update

        carried = (
            jnp.full((rows, 1), -1e30, jnp.float32),
            jnp.zeros((rows, 1), jnp.float32),
            jnp.zeros((rows, HEAD_DIM), jnp.float32),
        )
        last = block * parts + exp // span
        carried = lax.fori_loop(0, last, lambda index, now: step(index, now, False), carried)
        row_max, row_sum, weighted = step(last, carried, True)
        result = (weighted / row_sum).astype(jnp.bfloat16)
        for h in range(heads):
            out_ref[core, block, :, h * HEAD_DIM : (h + 1) * HEAD_DIM] = result[
                h * TOK_DEV : (h + 1) * TOK_DEV
            ]
        share(core, block).start()
        return unused

    def share(slot, block):
        return pltpu.make_async_remote_copy(
            src_ref=out_ref.at[slot, block],
            dst_ref=out_ref.at[slot, block],
            send_sem=out_send.at[block],
            recv_sem=out_recv.at[block],
            **at(exp=partner),
        )

    lax.fori_loop(0, seq_count, attend, 0)
    for d in range(1, seq_count):
        peer = flipped(seq, d)
        for half in range(2):
            kv_copy(half, peer, peer).wait_send()
        q_copy(peer, peer).wait_send()
    spread(exp, True, True, sent)
    relay(sent, False)
    for block in range(seq_count):
        share(core, block).wait_send()
        share(1 - core, block).wait_recv()

    @pl.when(chip + 1 < chips)
    def _():
        weight(0, exp + 2).wait_send()
        weight(1, partner).wait_recv()

    @pl.when(chip >= 1)
    def _():
        weight(1, exp - 2).wait_send()
        weight(0, partner).wait_recv()


def attention(queries, keys, values, proj_weight):
    seq_count, exp_count = lax.axis_size("seq"), lax.axis_size("exp")
    width = HEADS // seq_count * HEAD_DIM
    blocks = (seq_count, TOK_DEV, width)
    pairs = HEADS // seq_count * seq_count * TOK_DEV * exp_count * seq_count * TOK_DEV // 2
    vmem = pl.BlockSpec(memory_space=pltpu.VMEM)
    anywhere = pl.BlockSpec(memory_space=pl.ANY)
    dma = pltpu.SemaphoreType.DMA
    return pl.pallas_call(
        functools.partial(attention_kernel, seq_count, exp_count),
        out_shape=(
            jax.ShapeDtypeStruct((2, *blocks), jnp.bfloat16),
            jax.ShapeDtypeStruct((2, *proj_weight.shape), jnp.bfloat16),
        ),
        in_specs=[vmem, vmem, vmem, anywhere],
        out_specs=(vmem, anywhere),
        scratch_shapes=[
            pltpu.VMEM(blocks, jnp.bfloat16),
            pltpu.VMEM((exp_count, seq_count, TOK_DEV, 2 * HEAD_DIM), jnp.bfloat16),
            dma((2, seq_count)),
            dma((2, seq_count)),
            dma((seq_count,)),
            dma((seq_count,)),
            dma((3, exp_count)),
            dma((exp_count,)),
            dma((2,)),
            dma((2,)),
            dma((seq_count,)),
            dma((seq_count,)),
        ],
        compiler_params=pltpu.CompilerParams(
            collective_id=1, has_side_effects=True, vmem_limit_bytes=60 * 1024 * 1024
        ),
        cost_estimate=pl.CostEstimate(
            flops=pairs * 4 * HEAD_DIM, bytes_accessed=queries.size * 4, transcendentals=pairs
        ),
        name="attention",
    )(queries, keys, values, proj_weight)


def gather_lanes(ref, chunk, tiles):
    return jnp.concatenate([ref[chunk, :, t, :] for t in range(tiles)], axis=1)


def padded(rows):
    count = rows.shape[0]
    if count % PAD:
        rows = jnp.concatenate(
            [rows, jnp.zeros((PAD - count % PAD, rows.shape[1]), rows.dtype)], axis=0
        )
    return rows.astype(jnp.bfloat16)


def layer_kernel(
    seq_count,
    count,
    steps,
    depth,
    att_ref,
    res_ref,
    gain_ref,
    router_ref,
    sel_ref,
    first_ref,
    second_ref,
    named_ref,
    w_hbm,
    near_hbm,
    u_hbm,
    vg_hbm,
    ud_hbm,
    vd_hbm,
    out_ref,
    far_hbm,
    w_buf,
    part_send,
    part_recv,
    stream,
    u_buf,
    vg_buf,
    ud_buf,
    send,
    recv,
    back,
    send_x,
    recv_x,
    back_x,
    rank_sum,
    rank_in,
    square,
    token,
    mix_both,
    swap,
    swap_x,
    w_sem,
    load_sem,
    far_send,
    far_recv,
    part_send_sem,
    part_recv_sem,
    send_sem,
    recv_sem,
    send_x_sem,
    recv_x_sem,
    swap_sem,
):
    seq, me = lax.axis_index("seq"), lax.axis_index("exp")
    chips = count // 2
    chip, core = me // 2, me % 2
    pieces = count // EXPERTS
    piece_width = D // pieces
    block = D // count
    sub = block // PIECE
    width = 2 * PIECE
    tiles = width // 128
    total = chips * sub
    local = total // pieces
    unit = vg_buf.shape[-1]
    mine = me % pieces
    early = chip < (chips + 1) // 2
    rows_in = TOK_DEV * 2 * seq_count
    barrier, greetings = greet(seq_count, count)

    def chunk_of(i):
        return jnp.where(early, i, total - 1 - i)

    def columns(g):
        first = (g // sub) * 2 * block + (g % sub) * PIECE
        return first, first + block

    def span(start):
        return pl.ds(pl.multiple_of(start, 128), PIECE)

    def u_copies(l):
        return [
            pltpu.make_async_copy(
                u_hbm.at[0, pl.ds(pl.multiple_of(start - mine * piece_width, 128), PIECE)],
                u_buf.at[l, pl.ds(p * PIECE, PIECE)],
                w_sem.at[p, l],
            )
            for p, start in enumerate(columns(mine * local + l))
        ]

    def vd_copies(l):
        return [
            pltpu.make_async_copy(
                vd_hbm.at[0, :, span(start - mine * piece_width)],
                u_buf.at[l, pl.ds(0, RANK), pl.ds(p * PIECE, PIECE)],
                w_sem.at[2 + p, l],
            )
            for p, start in enumerate(columns(mine * local + l))
        ]

    def vg_copy(f):
        cols = pl.ds(pl.multiple_of(f * unit, unit), unit)
        return pltpu.make_async_copy(vg_hbm.at[0, :, :, cols], vg_buf.at[f % depth], w_sem.at[4, f])

    def ud_copy(f):
        rows = pl.ds(pl.multiple_of(f * unit, unit), unit)
        return pltpu.make_async_copy(ud_hbm.at[0, rows], ud_buf.at[f % depth], w_sem.at[5, f])

    def weight_hop(way, source, origin, h):
        return pltpu.make_async_remote_copy(
            src_ref=source,
            dst_ref=far_hbm.at[origin, h],
            send_sem=far_send.at[way, origin, h],
            recv_sem=far_recv.at[origin, h],
            **at(exp=me + 2 if way == 0 else me - 2),
        )

    inner = (chip >= 1) & (chip + 1 < chips)

    def start(copy):
        copy.start()

    def sent(copy):
        copy.wait_send()

    def near_hops(act):
        @pl.when(inner)
        def _():
            for h in range(sub):
                for way, k in ((0, sub - 1 - h), (1, h)):
                    source = near_hbm.at[way, :, pl.ds(k * PIECE, PIECE)]
                    act(weight_hop(way, source, chip - 1 if way == 0 else chip + 1, k))

    def far_arrival(origin, h):
        return pltpu.make_async_remote_copy(
            src_ref=far_hbm.at[origin, h],
            dst_ref=far_hbm.at[origin, h],
            send_sem=far_send.at[0, origin, h],
            recv_sem=far_recv.at[origin, h],
            **at(exp=flipped(me, 1)),
        )

    def pump(distance, h, act, wait):
        below, above = chip - distance, chip + distance

        @pl.when((below >= 0) & (chip + 1 < chips))
        def _():
            k = sub - 1 - h
            if wait:
                far_arrival(below, k).wait_recv()
            act(weight_hop(0, far_hbm.at[below, k], below, k))

        @pl.when((above < chips) & (chip >= 1))
        def _():
            if wait:
                far_arrival(above, h).wait_recv()
            act(weight_hop(1, far_hbm.at[above, h], above, h))

    pumps = [(distance, h) for distance in range(2, chips - 1) for h in range(sub)]

    def load(i):
        g = chunk_of(i)
        origin, h = g // sub, g % sub
        cols = span(h * PIECE)

        @pl.when(origin == chip)
        def _():
            pltpu.make_async_copy(w_hbm.at[:, cols], w_buf, load_sem).start()

        @pl.when(origin == chip - 1)
        def _():
            pltpu.make_async_copy(near_hbm.at[0, :, cols], w_buf, load_sem).start()

        @pl.when(origin == chip + 1)
        def _():
            pltpu.make_async_copy(near_hbm.at[1, :, cols], w_buf, load_sem).start()

        @pl.when((origin >= chip + 2) | (origin <= chip - 2))
        def _():
            @pl.when(((origin > chip) & (chip == 0)) | ((origin < chip) & (chip == chips - 1)))
            def _():
                far_arrival(origin, h).wait_recv()

            pltpu.make_async_copy(far_hbm.at[origin, h], w_buf, load_sem).start()

        pltpu.make_async_copy(w_hbm.at[:, cols], w_buf, load_sem).wait()

    def part_copy(i, d, t, block_from, core_from):
        peer, exp = flipped(seq, d), flipped(me, t)
        return pltpu.make_async_remote_copy(
            src_ref=part_send.at[i % (AHEAD + 1), exp % 2, peer],
            dst_ref=part_recv.at[i, core_from, block_from],
            send_sem=part_send_sem.at[i % (AHEAD + 1), exp % 2, peer],
            recv_sem=part_recv_sem.at[i, core_from, block_from],
            **at(seq=peer, exp=exp),
        )

    targets = [(d, t) for d in range(seq_count) for t in range(2) if d or t]

    def parts_sent(i):
        for d, t in targets:
            part_copy(i, d, t, seq, core).wait_send()

    def project(i):
        load(i)
        part = jnp.dot(
            att_ref[...].reshape(rows_in, att_ref.shape[-1]),
            w_buf[...],
            preferred_element_type=jnp.float32,
        )
        slot = i % (AHEAD + 1)
        part_send[slot] = part.astype(jnp.bfloat16).reshape(2, seq_count, TOK_DEV, PIECE)
        for d, t in targets:
            part_copy(i, d, t, seq, core).start()
        part_recv[i, core, seq] = part_send[slot, core, seq]

    def copies(phase, l, peer, slot, into, into_x):
        main = pltpu.make_async_remote_copy(
            src_ref=send.at[l, peer],
            dst_ref=into.at[l, slot],
            send_sem=send_sem.at[phase, l, peer],
            recv_sem=recv_sem.at[phase, l, slot],
            **at(exp=peer),
        )
        extra = pltpu.make_async_remote_copy(
            src_ref=send_x.at[l, peer],
            dst_ref=into_x.at[l, slot],
            send_sem=send_x_sem.at[phase, l, peer],
            recv_sem=recv_x_sem.at[phase, l, slot],
            **at(exp=peer),
        )
        return main, extra

    def send_chunk(phase, l, piece, into, into_x):
        for d in range(1, count):
            peer = flipped(me, d)

            def go():
                for copy in copies(phase, l, peer, me, into, into_x):
                    copy.start()

            if piece is None or pieces == 1:
                go()
            else:
                pl.when(peer % pieces == piece)(go)

        def keep():
            into[l, me] = send[l, me]
            into_x[l, me] = send_x[l, me]

        if piece is None or pieces == 1:
            keep()
        else:
            pl.when(mine == piece)(keep)

    def wait_sent(phase, l, into, into_x):
        for d in range(1, count):
            peer = flipped(me, d)
            for copy in copies(phase, l, peer, peer, into, into_x):
                copy.wait_send()

    def wait_got(phase, l, into, into_x, peers):
        for peer in peers:

            @pl.when(peer != me)
            def _():
                for copy in copies(phase, l, peer, peer, into, into_x):
                    copy.wait_recv()

    def finish(i):
        g = chunk_of(i)
        for d, t in targets:
            peer, exp = flipped(seq, d), flipped(me, t)
            part_copy(i, d, t, peer, exp % 2).wait_recv()
        halves = []
        for p, first in enumerate(columns(g)):
            update = part_recv[i, p, 0].astype(jnp.float32)
            for s in range(1, seq_count):
                update = update + part_recv[i, p, s].astype(jnp.float32)
            update = update.astype(jnp.bfloat16).astype(jnp.float32)
            value = res_ref[:, span(first)].astype(jnp.float32) + update
            stream[g, :, p * PIECE : (p + 1) * PIECE] = value
            token[0] += jnp.broadcast_to(
                jnp.sum(value * value, axis=-1, keepdims=True), (TOK_DEV, 128)
            )
            gained = (value * gain_ref[:, span(first)]).astype(jnp.bfloat16)
            token[1, :, :PAD] += lax.dot_general(
                gained,
                router_ref[:, span(first)],
                (((1,), (1,)), ((), ())),
                preferred_element_type=jnp.float32,
            )
            halves.append(value.astype(jnp.bfloat16))
        rows = jnp.dot(
            sel_ref[...], jnp.concatenate(halves, axis=1), preferred_element_type=jnp.float32
        )
        piece, l = g // local, g % local
        for k in range(EXPERTS):
            send[l, k * pieces + piece] = rows[k * MAIN : (k + 1) * MAIN].astype(jnp.bfloat16)
        extra = rows[EXPERTS * MAIN : EXPERTS * MAIN + EXPERTS]
        for t in range(tiles):
            lanes = extra[:, t * 128 : (t + 1) * 128]
            if pieces == 1:
                send_x[l, :, t, :] = lanes
            else:
                for k in range(EXPERTS):
                    send_x[l, k * pieces + piece, t : t + 1, :] = lanes[k : k + 1]
        send_chunk(0, l, piece, recv, recv_x)

    def weights_in():
        for l in range(local):
            for copy in u_copies(l):
                copy.start()
        for f in range(min(depth, steps)):
            vg_copy(f).start()
            ud_copy(f).start()

    pl.semaphore_wait(barrier, greetings)
    near_hops(start)
    weights_in()
    if len(pumps) > 2:
        for distance, h in pumps:
            pump(distance, h, start, True)
    token[...] = jnp.zeros_like(token)
    square[...] = jnp.zeros_like(square)
    rank_sum[...] = jnp.zeros_like(rank_sum)

    def first_half(i, carried):
        @pl.when(i < total)
        def _():
            @pl.when(i > AHEAD)
            def _():
                parts_sent(i - AHEAD - 1)

            project(i)

        @pl.when(i >= AHEAD)
        def _():
            finish(i - AHEAD)

        if len(pumps) <= 2:
            for place, (distance, h) in enumerate(pumps):

                @pl.when(i == AHEAD + 1 + place)
                def _():
                    pump(distance, h, start, True)

        return carried

    lax.fori_loop(0, total + AHEAD, first_half, 0)
    for i in range(total - AHEAD - 1, total):
        parts_sent(i)

    split = 2 * ((chips + 1) // 2)
    main_rows = count * MAIN

    def spread_gain(l):
        return jnp.concatenate(
            [gain_ref[:, span(start)] for start in columns(mine * local + l)], axis=1
        )

    def first_factor(t, carried):
        for low, high, l in ((0, split, t), (split, count, local - 1 - t)):
            wait_got(0, l, recv, recv_x, range(low, high))
            held = recv[l, low:high].reshape((high - low) * MAIN, width).astype(jnp.float32)
            extra = jnp.concatenate([recv_x[l, low:high, k, :] for k in range(tiles)], axis=1)
            fill = [jnp.zeros((low, width), jnp.float32)] if low else []
            rest = PAD - high
            fill += [extra] + ([jnp.zeros((rest, width), jnp.float32)] if rest else [])
            extra = jnp.concatenate(fill, axis=0) if len(fill) > 1 else extra
            rows = jnp.concatenate([held, extra], axis=0)
            squares = jnp.sum(rows * rows, axis=-1, keepdims=True)
            squares = jnp.broadcast_to(squares, (rows.shape[0], 128))
            gained = (rows * spread_gain(l)).astype(jnp.bfloat16)
            product = jnp.dot(gained, u_buf[l], preferred_element_type=jnp.float32)
            size = (high - low) * MAIN
            here = slice(low * MAIN, high * MAIN)
            square[here] += squares[:size]
            square[main_rows:] += squares[size:]
            rank_sum[here] += product[:size]
            rank_sum[main_rows:] += product[size:]
        return carried

    for l in range(local):
        for copy in u_copies(l):
            copy.wait()
    lax.fori_loop(0, local, first_factor, 0)
    for l in range(local):
        for copy in vd_copies(l):
            copy.start()

    def exchange(source, target, slot, bit):
        copy = pltpu.make_async_remote_copy(
            src_ref=source,
            dst_ref=target,
            send_sem=swap_sem.at[slot, 0],
            recv_sem=swap_sem.at[slot, 1],
            **at(exp=flipped(me, bit)),
        )
        copy.start()
        copy.wait()

    def add_pieces(slot, columns, with_square):
        bit = 1
        while bit < pieces:
            swap[slot, 0, :, :columns] = rank_sum[:, :columns].astype(jnp.bfloat16)
            exchange(swap.at[slot, 0], swap.at[slot, 1], 2 * slot, bit)
            rank_sum[:, :columns] += swap[slot, 1, :, :columns].astype(jnp.float32)
            if with_square:
                swap_x[slot, 0] = square[...]
                exchange(swap_x.at[slot, 0], swap_x.at[slot, 1], 2 * slot + 1, bit)
                square[...] += swap_x[slot, 1]
            bit *= 2
            slot += 1
        return slot

    slot = add_pieces(0, 2 * RANK, True)
    scale = lax.rsqrt(square[:, 0:1] * (1.0 / D) + EPS)
    rank_in[...] = (rank_sum[...] * scale).astype(jnp.bfloat16)
    rank_sum[:, :RANK] = jnp.zeros((rank_sum.shape[0], RANK), jnp.float32)

    def middle(f, carried):
        vg_copy(f).wait()
        ud_copy(f).wait()
        place = f % depth
        gate = jnp.dot(rank_in[:, :RANK], vg_buf[place, 0], preferred_element_type=jnp.float32)
        up = jnp.dot(rank_in[:, RANK:], vg_buf[place, 1], preferred_element_type=jnp.float32)
        hidden = (gate / (1.0 + jnp.exp(-gate)) * up).astype(jnp.bfloat16)
        rank_sum[:, :RANK] += jnp.dot(hidden, ud_buf[place], preferred_element_type=jnp.float32)

        @pl.when(f + depth < steps)
        def _():
            vg_copy(f + depth).start()
            ud_copy(f + depth).start()

        return carried

    lax.fori_loop(0, steps, middle, 0)
    add_pieces(slot, RANK, False)
    rank_in[:, :RANK] = rank_sum[:, :RANK].astype(jnp.bfloat16)

    def last_factor(l, carried):
        for copy in vd_copies(l):
            copy.wait()
        wait_sent(0, l, recv, recv_x)
        rows = jnp.dot(
            rank_in[:, :RANK], u_buf[l, :RANK, :width], preferred_element_type=jnp.float32
        )
        for k in range(count):
            send[l, k] = rows[k * MAIN : (k + 1) * MAIN].astype(jnp.bfloat16)
        extra = rows[main_rows : main_rows + count]
        for t in range(tiles):
            send_x[l, :, t, :] = extra[:, t * 128 : (t + 1) * 128]
        send_chunk(1, l, None, back, back_x)
        return carried

    lax.fori_loop(0, local, last_factor, 0)

    logits = token[1, :, :PAD] * lax.rsqrt(token[0, :, 0:1] * (1.0 / D) + EPS)
    first = jnp.sum(logits * named_ref[0], axis=-1, keepdims=True)
    second = jnp.sum(logits * named_ref[1], axis=-1, keepdims=True)
    mix = first_ref[...].astype(jnp.float32) / (1.0 + jnp.exp(second - first)) + second_ref[
        ...
    ].astype(jnp.float32) / (1.0 + jnp.exp(first - second))
    mix_high = mix.astype(jnp.bfloat16)
    mix_both[:TOK_DEV] = mix_high
    mix_both[TOK_DEV:] = (mix - mix_high.astype(jnp.float32)).astype(jnp.bfloat16)

    def combine(l, carried):
        wait_got(1, l, back, back_x, range(count))
        for piece in range(pieces):
            g = piece * local + l
            rows = back[l].reshape(EXPERTS, pieces, MAIN, width)[:, piece]
            extra = gather_lanes(back_x, l, tiles).reshape(EXPERTS, pieces, width)[:, piece]
            rows = jnp.concatenate([rows.reshape(EXPERTS * MAIN, width), padded(extra)], axis=0)
            both = jnp.dot(mix_both[...], rows, preferred_element_type=jnp.float32)
            result = (stream[g] + both[:TOK_DEV] + both[TOK_DEV:]).astype(jnp.bfloat16)
            for p, first in enumerate(columns(g)):
                out_ref[:, span(first)] = result[:, p * PIECE : (p + 1) * PIECE]
        return carried

    lax.fori_loop(0, local, combine, 0)

    def drain(l, carried):
        wait_sent(1, l, back, back_x)
        return carried

    lax.fori_loop(0, local, drain, 0)
    near_hops(sent)
    for distance, h in pumps:
        pump(distance, h, sent, False)


def layer(attended, residual, gain, router, select, first_at, second_at, named, weights):
    proj_weight, near, u_gate_up, v_gate_up, u_down, v_down = weights
    seq_count, count = lax.axis_size("seq"), lax.axis_size("exp")
    pieces = count // EXPERTS
    sub = D // count // PIECE
    total = count // 2 * sub
    local = total // pieces
    width = 2 * PIECE
    units = u_down.shape[1]
    unit = min(1024, units)
    steps = units // unit
    depth = min(5, max(1, steps - 2))
    rows = count * MAIN + PAD
    swaps = max(1, 2 * (pieces.bit_length() - 1))
    depth_in = proj_weight.shape[0]
    vmem = pl.BlockSpec(memory_space=pltpu.VMEM)
    anywhere = pl.BlockSpec(memory_space=pl.ANY)
    dma = pltpu.SemaphoreType.DMA
    half, full = jnp.bfloat16, jnp.float32
    block = (local, count, MAIN, width)
    block_x = (local, count, width // 128, 128)
    many = pieces > 1
    out, _ = pl.pallas_call(
        functools.partial(layer_kernel, seq_count, count, steps, depth),
        out_shape=(
            jax.ShapeDtypeStruct((TOK_DEV, D), half),
            jax.ShapeDtypeStruct((count // 2, sub, depth_in, PIECE), half),
        ),
        in_specs=[vmem] * 8 + [anywhere] * 6,
        out_specs=(vmem, anywhere),
        scratch_shapes=[
            pltpu.VMEM((depth_in, PIECE), half),
            pltpu.VMEM((AHEAD + 1, 2, seq_count, TOK_DEV, PIECE), half),
            pltpu.VMEM((total, 2, seq_count, TOK_DEV, PIECE), half),
            pltpu.VMEM((total, TOK_DEV, width), full),
            pltpu.VMEM((local, width, 2 * RANK), half),
            pltpu.VMEM((depth, 2, RANK, unit), half),
            pltpu.VMEM((depth, unit, RANK), half),
            pltpu.VMEM(block, half),
            pltpu.VMEM(block, half),
            pltpu.VMEM(block, half),
            pltpu.VMEM(block_x, full),
            pltpu.VMEM(block_x, full),
            pltpu.VMEM(block_x, full),
            pltpu.VMEM((rows, 2 * RANK), full),
            pltpu.VMEM((rows, 2 * RANK), half),
            pltpu.VMEM((rows, 128), full),
            pltpu.VMEM((2, TOK_DEV, 128), full),
            pltpu.VMEM((2 * TOK_DEV, select.shape[0]), half),
            pltpu.VMEM((swaps, 2, rows, 2 * RANK) if many else (1, 2, 16, 128), half),
            pltpu.VMEM((swaps, 2, rows, 128) if many else (1, 2, 8, 128), full),
            dma((6, max(local, steps))),
            dma(()),
            dma((2, count // 2, sub)),
            dma((count // 2, sub)),
            dma((AHEAD + 1, 2, seq_count)),
            dma((total, 2, seq_count)),
            dma((2, local, count)),
            dma((2, local, count)),
            dma((2, local, count)),
            dma((2, local, count)),
            dma((2 * swaps, 2)),
        ],
        compiler_params=pltpu.CompilerParams(
            collective_id=0, has_side_effects=True, vmem_limit_bytes=67043328
        ),
        cost_estimate=pl.CostEstimate(
            flops=rows * RANK * units * 6,
            bytes_accessed=units * RANK * 6,
            transcendentals=rows * units,
        ),
        name="layer",
    )(
        attended,
        residual,
        gain,
        router,
        select,
        first_at,
        second_at,
        named,
        proj_weight,
        near,
        u_gate_up,
        v_gate_up,
        u_down,
        v_down,
    )
    return out


def per_device(
    queries,
    keys,
    values,
    residual,
    proj_weight,
    norm_gain,
    router,
    expert_ids,
    u_gate_up,
    v_gate_up,
    u_down,
    v_down,
):
    attended, near = attention(queries, keys, values, proj_weight)
    expert_range = jnp.arange(EXPERTS, dtype=jnp.int32)
    flat_ids = expert_ids.reshape(TOK_DEV * 2)
    member = (flat_ids[:, None] == expert_range[None, :]).astype(jnp.int32)
    slot_of = jnp.sum((jnp.cumsum(member, axis=0) - 1) * member, axis=1)
    dest = jnp.where(
        slot_of < MAIN, flat_ids * MAIN + slot_of, EXPERTS * MAIN + flat_ids + (slot_of - MAIN)
    ).reshape(TOK_DEV, 2)
    places = jnp.arange(EXPERTS * MAIN + PAD, dtype=jnp.int32)
    first_at = (dest[:, 0:1] == places[None, :]).astype(jnp.bfloat16)
    second_at = (dest[:, 1:2] == places[None, :]).astype(jnp.bfloat16)
    select = (
        (dest[:, 0][None, :] == places[:, None]) | (dest[:, 1][None, :] == places[:, None])
    ).astype(jnp.bfloat16)
    named = (expert_ids.T[:, :, None] == jnp.arange(PAD, dtype=jnp.int32)).astype(jnp.float32)
    return layer(
        attended,
        residual,
        norm_gain.astype(jnp.float32)[None, :],
        jnp.pad(router.T, ((0, PAD - EXPERTS), (0, 0))),
        select,
        first_at,
        second_at,
        named,
        (proj_weight, near, u_gate_up, v_gate_up, u_down, v_down),
    )


def solution(mesh):
    in_specs = (
        P(("seq", "exp"), None),
        P(("seq", "exp"), None),
        P(("seq", "exp"), None),
        P(("seq", "exp"), None),
        P("seq", "exp"),
        P(),
        P(),
        P(("seq", "exp"), None),
        P("exp", None, None),
        P("exp", None, None, None),
        P("exp", None, None),
        P("exp", None, None),
    )
    out_specs = P(("seq", "exp"), None)
    return jax.shard_map(
        per_device, mesh=mesh, in_specs=in_specs, out_specs=out_specs, check_vma=False
    )
```

```python
import functools

import jax
import jax.numpy as jnp
from jax import lax
from jax.experimental import pallas as pl
from jax.experimental.pallas import tpu as pltpu
from jax.sharding import PartitionSpec as P

D = 6144
HEADS = 24
KV_HEADS = 4
HEAD_DIM = 128
EXPERTS = 8
RANK = 512
TOK_DEV = 128
CAP = 33


EPS = 1e-05
LOG2_E = 1.4426950408889634


MAIN = CAP // 16 * 16
PAD = 16
PIECE = 384
AHEAD = 3


def flipped(index, bits):
    bit = 1
    while bit <= bits:
        if bits & bit:
            index = index + bit * (1 - 2 * ((index // bit) % 2))
        bit *= 2
    return index


def at(**place):
    return {"device_id": place, "device_id_type": pl.DeviceIdType.MESH}


def greet(seq_count, exp_count):
    seq, exp = lax.axis_index("seq"), lax.axis_index("exp")
    barrier = pltpu.get_barrier_semaphore()
    for d in range(1, exp_count):
        pl.semaphore_signal(barrier, inc=1, **at(exp=flipped(exp, d)))
    for d in range(1, seq_count):
        for c in range(2):
            pl.semaphore_signal(
                barrier, inc=1, **at(seq=flipped(seq, d), exp=flipped(exp, c))
            )
    return barrier, exp_count - 1 + 2 * (seq_count - 1)


MAIN = CAP // 16 * 16
PAD = 16
PIECE = 384
AHEAD = 3


def flipped(index, bits):
    bit = 1
    while bit <= bits:
        if bits & bit:
            index = index + bit * (1 - 2 * ((index // bit) % 2))
        bit *= 2
    return index


def at(**place):
    return {"device_id": place, "device_id_type": pl.DeviceIdType.MESH}


def greet(seq_count, exp_count):
    seq, exp = lax.axis_index("seq"), lax.axis_index("exp")
    barrier = pltpu.get_barrier_semaphore()
    for d in range(1, exp_count):
        pl.semaphore_signal(barrier, inc=1, **at(exp=flipped(exp, d)))
    for d in range(1, seq_count):
        for c in range(2):
            pl.semaphore_signal(
                barrier, inc=1, **at(seq=flipped(seq, d), exp=flipped(exp, c))
            )
    return barrier, exp_count - 1 + 2 * (seq_count - 1)


def attention_kernel(
    seq_count,
    exp_count,
    q_ref,
    k_ref,
    v_ref,
    w_hbm,
    out_ref,
    near_hbm,
    q_all,
    kv_all,
    in_send,
    in_recv,
    q_send,
    q_recv,
    kv_send,
    kv_recv,
    w_send,
    w_recv,
    out_send,
    out_recv,
):
    seq, exp = lax.axis_index("seq"), lax.axis_index("exp")
    chips = exp_count // 2
    chip, core = exp // 2, exp % 2
    heads = HEADS // seq_count
    width = heads * HEAD_DIM
    shares = max(1, seq_count // KV_HEADS)
    barrier, greetings = greet(seq_count, exp_count)
    own = pl.ds(pl.multiple_of((seq // shares) * HEAD_DIM, HEAD_DIM), HEAD_DIM)
    kv_all[exp, seq, :, :HEAD_DIM] = k_ref[:, own]
    kv_all[exp, seq, :, HEAD_DIM:] = v_ref[:, own]
    q_all[seq] = q_ref[:, pl.ds(pl.multiple_of(seq * width, width), width)]
    pl.semaphore_wait(barrier, greetings)

    def kv_copy(half, peer, block):
        ref = (k_ref, v_ref)[half]
        head = pl.ds(pl.multiple_of((peer // shares) * HEAD_DIM, HEAD_DIM), HEAD_DIM)
        return pltpu.make_async_remote_copy(
            src_ref=ref.at[:, head],
            dst_ref=kv_all.at[exp, block, :, pl.ds(half * HEAD_DIM, HEAD_DIM)],
            send_sem=in_send.at[half, peer],
            recv_sem=in_recv.at[half, block],
            **at(seq=peer),
        )

    def q_copy(peer, block):
        return pltpu.make_async_remote_copy(
            src_ref=q_ref.at[:, pl.ds(pl.multiple_of(peer * width, width), width)],
            dst_ref=q_all.at[block],
            send_sem=q_send.at[peer],
            recv_sem=q_recv.at[block],
            **at(seq=peer),
        )

    for d in range(1, seq_count):
        for half in range(2):
            kv_copy(half, flipped(seq, d), seq).start()
    for d in range(1, seq_count):
        q_copy(flipped(seq, d), seq).start()

    def pass_on(way, block, target):
        return pltpu.make_async_remote_copy(
            src_ref=kv_all.at[block],
            dst_ref=kv_all.at[block],
            send_sem=kv_send.at[way, block],
            recv_sem=kv_recv.at[block],
            **at(exp=target),
        )

    cut_rows = w_hbm.shape[0] // 2
    sub = w_hbm.shape[1] // PIECE

    def weight(way, target, u):
        h = sub - 1 - u // 2 if way == 0 else u // 2
        rows = pl.ds((u % 2) * cut_rows, cut_rows)
        return pltpu.make_async_remote_copy(
            src_ref=w_hbm.at[rows, pl.ds(h * PIECE, PIECE)],
            dst_ref=near_hbm.at[way, h, rows],
            send_sem=w_send.at[way, u],
            recv_sem=w_recv.at[way, u],
            **at(exp=target),
        )

    def weights(low, high):
        @pl.when(chip + 1 < chips)
        def _():
            for u in range(low, high):
                weight(0, exp + 2, u).start()

        @pl.when(chip >= 1)
        def _():
            for u in range(low, high):
                weight(1, exp - 2, u).start()

    weights(0, 1)

    partner = flipped(exp, 1)

    def spread(block, up, down, act):
        if up:

            @pl.when(chip + 1 < chips)
            def _():
                act(pass_on(0, block, exp + 2))

        if down:

            @pl.when(chip >= 1)
            def _():
                act(pass_on(1, block, exp - 2))

        act(pass_on(2, block, partner))

    def start(copy):
        copy.start()

    def sent(copy):
        copy.wait_send()

    for d in range(1, seq_count):
        for half in range(2):
            peer = flipped(seq, d)
            kv_copy(half, peer, peer).wait_recv()
    spread(exp, True, True, start)

    def relay(act, wait):
        for hop in range(1, chips):
            below, above = exp - 2 * hop, exp + 2 * hop

            @pl.when(chip >= hop)
            def _():
                if wait:
                    pass_on(2, below, partner).wait_recv()
                spread(below, True, False, act)

            @pl.when(chip + hop < chips)
            def _():
                if wait:
                    pass_on(2, above, partner).wait_recv()
                spread(above, False, True, act)

    relay(start, True)

    weights(1, 2 * sub)

    for other in range(chips):
        pass_on(2, 2 * other + 1 - core, partner).wait_recv()
    for d in range(1, seq_count):
        peer = flipped(seq, d)
        q_copy(peer, peer).wait_recv()

    parts = max(1, exp_count * TOK_DEV // 512)
    span = exp_count // parts
    chunk = span * TOK_DEV
    rows = heads * TOK_DEV

    def attend(block, unused):
        query = jnp.concatenate(
            [q_all[block, :, h * HEAD_DIM : (h + 1) * HEAD_DIM] for h in range(heads)], axis=0
        )

        def step(index, carried, masked):
            row_max, row_sum, weighted = carried
            held = kv_all[pl.ds((index % parts) * span, span), index // parts]
            held = held.reshape(chunk, 2 * HEAD_DIM)
            scores = lax.dot_general(
                query,
                held[:, :HEAD_DIM],
                (((1,), (1,)), ((), ())),
                preferred_element_type=jnp.float32,
            ) * (HEAD_DIM ** (-0.5) * LOG2_E)
            if masked:
                offset = (exp % span) * TOK_DEV
                mine = lax.broadcasted_iota(jnp.int32, (rows, chunk), 0) % TOK_DEV + offset
                other = lax.broadcasted_iota(jnp.int32, (rows, chunk), 1)
                scores = jnp.where(other <= mine, scores, -jnp.inf)
            new_max = jnp.maximum(row_max, jnp.max(scores, axis=-1, keepdims=True))
            fading = jnp.exp2(row_max - new_max)
            terms = jnp.exp2(scores - new_max)
            row_sum = row_sum * fading + jnp.sum(terms, axis=-1, keepdims=True)
            update = jnp.dot(
                terms.astype(jnp.bfloat16), held[:, HEAD_DIM:], preferred_element_type=jnp.float32
            )
            return new_max, row_sum, weighted * fading + update

        carried = (
            jnp.full((rows, 1), -1e30, jnp.float32),
            jnp.zeros((rows, 1), jnp.float32),
            jnp.zeros((rows, HEAD_DIM), jnp.float32),
        )
        last = block * parts + exp // span
        carried = lax.fori_loop(0, last, lambda index, now: step(index, now, False), carried)
        row_max, row_sum, weighted = step(last, carried, True)
        result = (weighted / row_sum).astype(jnp.bfloat16)
        for h in range(heads):
            out_ref[core, block, :, h * HEAD_DIM : (h + 1) * HEAD_DIM] = result[
                h * TOK_DEV : (h + 1) * TOK_DEV
            ]
        share(core, block).start()
        return unused

    def share(slot, block):
        return pltpu.make_async_remote_copy(
            src_ref=out_ref.at[slot, block],
            dst_ref=out_ref.at[slot, block],
            send_sem=out_send.at[block],
            recv_sem=out_recv.at[block],
            **at(exp=partner),
        )

    lax.fori_loop(0, seq_count, attend, 0)
    for d in range(1, seq_count):
        peer = flipped(seq, d)
        for half in range(2):
            kv_copy(half, peer, peer).wait_send()
        q_copy(peer, peer).wait_send()
    spread(exp, True, True, sent)
    relay(sent, False)
    for block in range(seq_count):
        share(core, block).wait_send()
        share(1 - core, block).wait_recv()

    @pl.when(chip + 1 < chips)
    def _():
        for u in range(2 * sub):
            weight(0, exp + 2, u).wait_send()
            weight(1, partner, u).wait_recv()

    @pl.when(chip >= 1)
    def _():
        for u in range(2 * sub):
            weight(1, exp - 2, u).wait_send()
            weight(0, partner, u).wait_recv()


def attention(queries, keys, values, proj_weight):
    seq_count, exp_count = lax.axis_size("seq"), lax.axis_size("exp")
    width = HEADS // seq_count * HEAD_DIM
    blocks = (seq_count, TOK_DEV, width)
    pairs = HEADS // seq_count * seq_count * TOK_DEV * exp_count * seq_count * TOK_DEV // 2
    vmem = pl.BlockSpec(memory_space=pltpu.VMEM)
    anywhere = pl.BlockSpec(memory_space=pl.ANY)
    dma = pltpu.SemaphoreType.DMA
    return pl.pallas_call(
        functools.partial(attention_kernel, seq_count, exp_count),
        out_shape=(
            jax.ShapeDtypeStruct((2, *blocks), jnp.bfloat16),
            jax.ShapeDtypeStruct(
                (2, proj_weight.shape[1] // PIECE, proj_weight.shape[0], PIECE), jnp.bfloat16
            ),
        ),
        in_specs=[vmem, vmem, vmem, anywhere],
        out_specs=(vmem, anywhere),
        scratch_shapes=[
            pltpu.VMEM(blocks, jnp.bfloat16),
            pltpu.VMEM((exp_count, seq_count, TOK_DEV, 2 * HEAD_DIM), jnp.bfloat16),
            dma((2, seq_count)),
            dma((2, seq_count)),
            dma((seq_count,)),
            dma((seq_count,)),
            dma((3, exp_count)),
            dma((exp_count,)),
            dma((2, proj_weight.shape[1] // PIECE * 2)),
            dma((2, proj_weight.shape[1] // PIECE * 2)),
            dma((seq_count,)),
            dma((seq_count,)),
        ],
        compiler_params=pltpu.CompilerParams(
            collective_id=1, has_side_effects=True, vmem_limit_bytes=60 * 1024 * 1024
        ),
        cost_estimate=pl.CostEstimate(
            flops=pairs * 4 * HEAD_DIM, bytes_accessed=queries.size * 4, transcendentals=pairs
        ),
        name="attention",
    )(queries, keys, values, proj_weight)


def gather_lanes(ref, chunk, tiles):
    return jnp.concatenate([ref[chunk, :, t, :] for t in range(tiles)], axis=1)


def padded(rows):
    count = rows.shape[0]
    if count % PAD:
        rows = jnp.concatenate(
            [rows, jnp.zeros((PAD - count % PAD, rows.shape[1]), rows.dtype)], axis=0
        )
    return rows.astype(jnp.bfloat16)


def layer_kernel(
    seq_count,
    count,
    steps,
    depth,
    att_ref,
    res_ref,
    gain_ref,
    router_ref,
    sel_ref,
    first_ref,
    second_ref,
    named_ref,
    w_hbm,
    near_hbm,
    u_hbm,
    vg_hbm,
    ud_hbm,
    vd_hbm,
    out_ref,
    far_hbm,
    w_buf,
    part_send,
    part_recv,
    stream,
    u_buf,
    vg_buf,
    ud_buf,
    send,
    recv,
    back,
    send_x,
    recv_x,
    back_x,
    rank_sum,
    rank_in,
    square,
    token,
    mix_both,
    swap,
    swap_x,
    w_sem,
    load_sem,
    far_send,
    far_recv,
    part_send_sem,
    part_recv_sem,
    send_sem,
    recv_sem,
    send_x_sem,
    recv_x_sem,
    swap_sem,
):
    seq, me = lax.axis_index("seq"), lax.axis_index("exp")
    chips = count // 2
    chip, core = me // 2, me % 2
    pieces = count // EXPERTS
    piece_width = D // pieces
    block = D // count
    sub = block // PIECE
    width = 2 * PIECE
    tiles = width // 128
    total = chips * sub
    local = total // pieces
    unit = vg_buf.shape[-1]
    mine = me % pieces
    early = chip < (chips + 1) // 2
    rows_in = TOK_DEV * 2 * seq_count
    barrier, greetings = greet(seq_count, count)

    def chunk_of(i):
        return jnp.where(early, i, total - 1 - i)

    def columns(g):
        first = (g // sub) * 2 * block + (g % sub) * PIECE
        return first, first + block

    def span(start):
        return pl.ds(pl.multiple_of(start, 128), PIECE)

    def u_copies(l):
        return [
            pltpu.make_async_copy(
                u_hbm.at[0, pl.ds(pl.multiple_of(start - mine * piece_width, 128), PIECE)],
                u_buf.at[l, pl.ds(p * PIECE, PIECE)],
                w_sem.at[p, l],
            )
            for p, start in enumerate(columns(mine * local + l))
        ]

    def vd_copies(l):
        return [
            pltpu.make_async_copy(
                vd_hbm.at[0, :, span(start - mine * piece_width)],
                u_buf.at[l, pl.ds(0, RANK), pl.ds(p * PIECE, PIECE)],
                w_sem.at[2 + p, l],
            )
            for p, start in enumerate(columns(mine * local + l))
        ]

    def vg_copy(f):
        cols = pl.ds(pl.multiple_of(f * unit, unit), unit)
        return pltpu.make_async_copy(vg_hbm.at[0, :, :, cols], vg_buf.at[f % depth], w_sem.at[4, f])

    def ud_copy(f):
        rows = pl.ds(pl.multiple_of(f * unit, unit), unit)
        return pltpu.make_async_copy(ud_hbm.at[0, rows], ud_buf.at[f % depth], w_sem.at[5, f])

    cut_rows = w_hbm.shape[0] // 2
    units = 2 * sub

    def part_of(way, u):
        h = sub - 1 - u // 2 if way == 0 else u // 2
        return h, pl.ds((u % 2) * cut_rows, cut_rows), u % 2

    def weight_hop(way, origin, u, near):
        h, rows, r = part_of(way, u)
        target = far_hbm.at[origin, h, rows]
        return pltpu.make_async_remote_copy(
            src_ref=near_hbm.at[way, h, rows] if near else target,
            dst_ref=target,
            send_sem=far_send.at[way, origin, h, r],
            recv_sem=far_recv.at[origin, h, r],
            **at(exp=me + 2 if way == 0 else me - 2),
        )

    def far_arrival(origin, h, r):
        target = far_hbm.at[origin, h, pl.ds(r * cut_rows, cut_rows)]
        return pltpu.make_async_remote_copy(
            src_ref=target,
            dst_ref=target,
            send_sem=far_send.at[0, origin, h, r],
            recv_sem=far_recv.at[origin, h, r],
            **at(exp=flipped(me, 1)),
        )

    def pump(j, act, wait):
        distance, u = j // units, j % units
        below, above = chip - distance, chip + distance

        @pl.when((below >= 0) & (chip + 1 < chips))
        def _():
            if wait and distance > 1:
                h, _, r = part_of(0, u)
                far_arrival(below, h, r).wait_recv()
            act(weight_hop(0, below, u, distance == 1))

        @pl.when((above < chips) & (chip >= 1))
        def _():
            if wait and distance > 1:
                h, _, r = part_of(1, u)
                far_arrival(above, h, r).wait_recv()
            act(weight_hop(1, above, u, distance == 1))

    pump_count = (chips - 1) * units

    def start(copy):
        copy.start()

    def sent(copy):
        copy.wait_send()

    def load(i):
        g = chunk_of(i)
        origin, h = g // sub, g % sub

        @pl.when(origin == chip)
        def _():
            pltpu.make_async_copy(w_hbm.at[:, span(h * PIECE)], w_buf, load_sem).start()

        @pl.when(origin == chip - 1)
        def _():
            pltpu.make_async_copy(near_hbm.at[0, h], w_buf, load_sem).start()

        @pl.when(origin == chip + 1)
        def _():
            pltpu.make_async_copy(near_hbm.at[1, h], w_buf, load_sem).start()

        @pl.when((origin >= chip + 2) | (origin <= chip - 2))
        def _():
            @pl.when(((origin > chip) & (chip == 0)) | ((origin < chip) & (chip == chips - 1)))
            def _():
                for r in range(2):
                    far_arrival(origin, h, r).wait_recv()

            pltpu.make_async_copy(far_hbm.at[origin, h], w_buf, load_sem).start()

        pltpu.make_async_copy(near_hbm.at[0, h], w_buf, load_sem).wait()

    def part_copy(i, d, t, block_from, core_from):
        peer, exp = flipped(seq, d), flipped(me, t)
        return pltpu.make_async_remote_copy(
            src_ref=part_send.at[i % (AHEAD + 1), exp % 2, peer],
            dst_ref=part_recv.at[i, core_from, block_from],
            send_sem=part_send_sem.at[i % (AHEAD + 1), exp % 2, peer],
            recv_sem=part_recv_sem.at[i, core_from, block_from],
            **at(seq=peer, exp=exp),
        )

    targets = [(d, t) for d in range(seq_count) for t in range(2) if d or t]

    def parts_sent(i):
        for d, t in targets:
            part_copy(i, d, t, seq, core).wait_send()

    def project(i):
        load(i)
        part = jnp.dot(
            att_ref[...].reshape(rows_in, att_ref.shape[-1]),
            w_buf[...],
            preferred_element_type=jnp.float32,
        )
        slot = i % (AHEAD + 1)
        part_send[slot] = part.astype(jnp.bfloat16).reshape(2, seq_count, TOK_DEV, PIECE)
        for d, t in targets:
            part_copy(i, d, t, seq, core).start()
        part_recv[i, core, seq] = part_send[slot, core, seq]

    def copies(phase, l, peer, slot, into, into_x):
        main = pltpu.make_async_remote_copy(
            src_ref=send.at[l, peer],
            dst_ref=into.at[l, slot],
            send_sem=send_sem.at[phase, l, peer],
            recv_sem=recv_sem.at[phase, l, slot],
            **at(exp=peer),
        )
        extra = pltpu.make_async_remote_copy(
            src_ref=send_x.at[l, peer],
            dst_ref=into_x.at[l, slot],
            send_sem=send_x_sem.at[phase, l, peer],
            recv_sem=recv_x_sem.at[phase, l, slot],
            **at(exp=peer),
        )
        return main, extra

    def send_chunk(phase, l, piece, into, into_x):
        for d in range(1, count):
            peer = flipped(me, d)

            def go():
                for copy in copies(phase, l, peer, me, into, into_x):
                    copy.start()

            if piece is None or pieces == 1:
                go()
            else:
                pl.when(peer % pieces == piece)(go)

        def keep():
            into[l, me] = send[l, me]
            into_x[l, me] = send_x[l, me]

        if piece is None or pieces == 1:
            keep()
        else:
            pl.when(mine == piece)(keep)

    def wait_sent(phase, l, into, into_x):
        for d in range(1, count):
            peer = flipped(me, d)
            for copy in copies(phase, l, peer, peer, into, into_x):
                copy.wait_send()

    def wait_got(phase, l, into, into_x, peers):
        for peer in peers:

            @pl.when(peer != me)
            def _():
                for copy in copies(phase, l, peer, peer, into, into_x):
                    copy.wait_recv()

    def finish(i):
        g = chunk_of(i)
        for d, t in targets:
            peer, exp = flipped(seq, d), flipped(me, t)
            part_copy(i, d, t, peer, exp % 2).wait_recv()
        halves = []
        for p, first in enumerate(columns(g)):
            update = part_recv[i, p, 0].astype(jnp.float32)
            for s in range(1, seq_count):
                update = update + part_recv[i, p, s].astype(jnp.float32)
            update = update.astype(jnp.bfloat16).astype(jnp.float32)
            value = res_ref[:, span(first)].astype(jnp.float32) + update
            stream[g, :, p * PIECE : (p + 1) * PIECE] = value
            token[0] += jnp.broadcast_to(
                jnp.sum(value * value, axis=-1, keepdims=True), (TOK_DEV, 128)
            )
            gained = (value * gain_ref[:, span(first)]).astype(jnp.bfloat16)
            token[1, :, :EXPERTS] += lax.dot_general(
                gained,
                router_ref[:, span(first)],
                (((1,), (1,)), ((), ())),
                preferred_element_type=jnp.float32,
            )
            halves.append(value.astype(jnp.bfloat16))
        rows = jnp.dot(
            sel_ref[...], jnp.concatenate(halves, axis=1), preferred_element_type=jnp.float32
        )
        piece, l = g // local, g % local
        for k in range(EXPERTS):
            send[l, k * pieces + piece] = rows[k * MAIN : (k + 1) * MAIN].astype(jnp.bfloat16)
        extra = rows[EXPERTS * MAIN : EXPERTS * MAIN + EXPERTS]
        for t in range(tiles):
            lanes = extra[:, t * 128 : (t + 1) * 128]
            if pieces == 1:
                send_x[l, :, t, :] = lanes
            else:
                for k in range(EXPERTS):
                    send_x[l, k * pieces + piece, t : t + 1, :] = lanes[k : k + 1]
        send_chunk(0, l, piece, recv, recv_x)

    def weights_in():
        for l in range(local):
            for copy in u_copies(l):
                copy.start()
        for f in range(min(depth, steps)):
            vg_copy(f).start()
            ud_copy(f).start()

    pl.semaphore_wait(barrier, greetings)
    for j in range(units, 2 * units):
        pump(j, start, True)
    rest = list(range(2 * units, pump_count))
    if len(rest) > 4:
        for j in rest:
            pump(j, start, True)
        rest = []
    token[...] = jnp.zeros_like(token)
    square[...] = jnp.zeros_like(square)
    rank_sum[...] = jnp.zeros_like(rank_sum)

    def first_half(i, carried):
        @pl.when(i < total)
        def _():
            @pl.when(i > AHEAD)
            def _():
                parts_sent(i - AHEAD - 1)

            project(i)

        @pl.when(i == min(AHEAD, total - 1))
        def _():
            weights_in()

        @pl.when(i == AHEAD)
        def _():
            for j in rest:
                pump(j, start, True)

        @pl.when(i >= AHEAD)
        def _():
            finish(i - AHEAD)

        return carried

    lax.fori_loop(0, total + AHEAD, first_half, 0)
    for i in range(total - AHEAD - 1, total):
        parts_sent(i)

    split = 2 * ((chips + 1) // 2)
    main_rows = count * MAIN

    def spread_gain(l):
        return jnp.concatenate(
            [gain_ref[:, span(start)] for start in columns(mine * local + l)], axis=1
        )

    def first_factor(t, carried):
        for low, high, l in ((0, split, t), (split, count, local - 1 - t)):
            wait_got(0, l, recv, recv_x, range(low, high))
            held = recv[l, low:high].reshape((high - low) * MAIN, width).astype(jnp.float32)
            extra = jnp.concatenate([recv_x[l, low:high, k, :] for k in range(tiles)], axis=1)
            fill = [jnp.zeros((low, width), jnp.float32)] if low else []
            rest = PAD - high
            fill += [extra] + ([jnp.zeros((rest, width), jnp.float32)] if rest else [])
            extra = jnp.concatenate(fill, axis=0) if len(fill) > 1 else extra
            rows = jnp.concatenate([held, extra], axis=0)
            squares = jnp.sum(rows * rows, axis=-1, keepdims=True)
            squares = jnp.broadcast_to(squares, (rows.shape[0], 128))
            gained = (rows * spread_gain(l)).astype(jnp.bfloat16)
            product = jnp.dot(gained, u_buf[l], preferred_element_type=jnp.float32)
            size = (high - low) * MAIN
            here = slice(low * MAIN, high * MAIN)
            square[here] += squares[:size]
            square[main_rows:] += squares[size:]
            rank_sum[here] += product[:size]
            rank_sum[main_rows:] += product[size:]
        return carried

    for l in range(local):
        for copy in u_copies(l):
            copy.wait()
    lax.fori_loop(0, local, first_factor, 0)
    for l in range(local):
        for copy in vd_copies(l):
            copy.start()

    def exchange(source, target, slot, bit):
        copy = pltpu.make_async_remote_copy(
            src_ref=source,
            dst_ref=target,
            send_sem=swap_sem.at[slot, 0],
            recv_sem=swap_sem.at[slot, 1],
            **at(exp=flipped(me, bit)),
        )
        copy.start()
        copy.wait()

    def add_pieces(slot, columns, with_square):
        bit = 1
        while bit < pieces:
            swap[slot, 0, :, :columns] = rank_sum[:, :columns].astype(jnp.bfloat16)
            exchange(swap.at[slot, 0], swap.at[slot, 1], 2 * slot, bit)
            rank_sum[:, :columns] += swap[slot, 1, :, :columns].astype(jnp.float32)
            if with_square:
                swap_x[slot, 0] = square[...]
                exchange(swap_x.at[slot, 0], swap_x.at[slot, 1], 2 * slot + 1, bit)
                square[...] += swap_x[slot, 1]
            bit *= 2
            slot += 1
        return slot

    slot = add_pieces(0, 2 * RANK, True)
    scale = lax.rsqrt(square[:, 0:1] * (1.0 / D) + EPS)
    rank_in[...] = (rank_sum[...] * scale).astype(jnp.bfloat16)
    rank_sum[:, :RANK] = jnp.zeros((rank_sum.shape[0], RANK), jnp.float32)

    def middle(f, carried):
        vg_copy(f).wait()
        ud_copy(f).wait()
        place = f % depth
        gate = jnp.dot(rank_in[:, :RANK], vg_buf[place, 0], preferred_element_type=jnp.float32)
        up = jnp.dot(rank_in[:, RANK:], vg_buf[place, 1], preferred_element_type=jnp.float32)
        hidden = (gate / (1.0 + jnp.exp(-gate)) * up).astype(jnp.bfloat16)
        rank_sum[:, :RANK] += jnp.dot(hidden, ud_buf[place], preferred_element_type=jnp.float32)

        @pl.when(f + depth < steps)
        def _():
            vg_copy(f + depth).start()
            ud_copy(f + depth).start()

        return carried

    lax.fori_loop(0, steps, middle, 0)
    add_pieces(slot, RANK, False)
    rank_in[:, :RANK] = rank_sum[:, :RANK].astype(jnp.bfloat16)

    def last_factor(l, carried):
        for copy in vd_copies(l):
            copy.wait()
        wait_sent(0, l, recv, recv_x)
        rows = jnp.dot(
            rank_in[:, :RANK], u_buf[l, :RANK, :width], preferred_element_type=jnp.float32
        )
        for k in range(count):
            send[l, k] = rows[k * MAIN : (k + 1) * MAIN].astype(jnp.bfloat16)
        extra = rows[main_rows : main_rows + count]
        for t in range(tiles):
            send_x[l, :, t, :] = extra[:, t * 128 : (t + 1) * 128]
        send_chunk(1, l, None, back, back_x)
        return carried

    lax.fori_loop(0, local, last_factor, 0)

    logits = token[1, :, :EXPERTS] * lax.rsqrt(token[0, :, 0:1] * (1.0 / D) + EPS)
    first = jnp.sum(logits * named_ref[0], axis=-1, keepdims=True)
    second = jnp.sum(logits * named_ref[1], axis=-1, keepdims=True)
    mix = first_ref[...].astype(jnp.float32) / (1.0 + jnp.exp(second - first)) + second_ref[
        ...
    ].astype(jnp.float32) / (1.0 + jnp.exp(first - second))
    mix_high = mix.astype(jnp.bfloat16)
    mix_both[:TOK_DEV] = mix_high
    mix_both[TOK_DEV:] = (mix - mix_high.astype(jnp.float32)).astype(jnp.bfloat16)

    def combine(l, carried):
        wait_got(1, l, back, back_x, range(count))
        for piece in range(pieces):
            g = piece * local + l
            rows = back[l].reshape(EXPERTS, pieces, MAIN, width)[:, piece]
            extra = gather_lanes(back_x, l, tiles).reshape(EXPERTS, pieces, width)[:, piece]
            rows = jnp.concatenate([rows.reshape(EXPERTS * MAIN, width), padded(extra)], axis=0)
            both = jnp.dot(mix_both[...], rows, preferred_element_type=jnp.float32)
            result = (stream[g] + both[:TOK_DEV] + both[TOK_DEV:]).astype(jnp.bfloat16)
            for p, first in enumerate(columns(g)):
                out_ref[:, span(first)] = result[:, p * PIECE : (p + 1) * PIECE]
        return carried

    lax.fori_loop(0, local, combine, 0)

    def drain(l, carried):
        wait_sent(1, l, back, back_x)
        return carried

    lax.fori_loop(0, local, drain, 0)
    for j in range(units, pump_count):
        pump(j, sent, False)


def layer(attended, residual, gain, router, select, first_at, second_at, named, weights):
    proj_weight, near, u_gate_up, v_gate_up, u_down, v_down = weights
    seq_count, count = lax.axis_size("seq"), lax.axis_size("exp")
    pieces = count // EXPERTS
    sub = D // count // PIECE
    total = count // 2 * sub
    local = total // pieces
    width = 2 * PIECE
    units = u_down.shape[1]
    unit = min(1024, units)
    steps = units // unit
    depth = min(5, max(1, steps - 2))
    rows = count * MAIN + PAD
    swaps = max(1, 2 * (pieces.bit_length() - 1))
    depth_in = proj_weight.shape[0]
    vmem = pl.BlockSpec(memory_space=pltpu.VMEM)
    anywhere = pl.BlockSpec(memory_space=pl.ANY)
    dma = pltpu.SemaphoreType.DMA
    half, full = jnp.bfloat16, jnp.float32
    block = (local, count, MAIN, width)
    block_x = (local, count, width // 128, 128)
    many = pieces > 1
    out, _ = pl.pallas_call(
        functools.partial(layer_kernel, seq_count, count, steps, depth),
        out_shape=(
            jax.ShapeDtypeStruct((TOK_DEV, D), half),
            jax.ShapeDtypeStruct((count // 2, sub, depth_in, PIECE), half),
        ),
        in_specs=[vmem] * 8 + [anywhere] * 6,
        out_specs=(vmem, anywhere),
        scratch_shapes=[
            pltpu.VMEM((depth_in, PIECE), half),
            pltpu.VMEM((AHEAD + 1, 2, seq_count, TOK_DEV, PIECE), half),
            pltpu.VMEM((total, 2, seq_count, TOK_DEV, PIECE), half),
            pltpu.VMEM((total, TOK_DEV, width), full),
            pltpu.VMEM((local, width, 2 * RANK), half),
            pltpu.VMEM((depth, 2, RANK, unit), half),
            pltpu.VMEM((depth, unit, RANK), half),
            pltpu.VMEM(block, half),
            pltpu.VMEM(block, half),
            pltpu.VMEM(block, half),
            pltpu.VMEM(block_x, full),
            pltpu.VMEM(block_x, full),
            pltpu.VMEM(block_x, full),
            pltpu.VMEM((rows, 2 * RANK), full),
            pltpu.VMEM((rows, 2 * RANK), half),
            pltpu.VMEM((rows, 128), full),
            pltpu.VMEM((2, TOK_DEV, 128), full),
            pltpu.VMEM((2 * TOK_DEV, select.shape[0]), half),
            pltpu.VMEM((swaps, 2, rows, 2 * RANK) if many else (1, 2, 16, 128), half),
            pltpu.VMEM((swaps, 2, rows, 128) if many else (1, 2, 8, 128), full),
            dma((6, max(local, steps))),
            dma(()),
            dma((2, count // 2, sub, 2)),
            dma((count // 2, sub, 2)),
            dma((AHEAD + 1, 2, seq_count)),
            dma((total, 2, seq_count)),
            dma((2, local, count)),
            dma((2, local, count)),
            dma((2, local, count)),
            dma((2, local, count)),
            dma((2 * swaps, 2)),
        ],
        compiler_params=pltpu.CompilerParams(
            collective_id=0, has_side_effects=True, vmem_limit_bytes=67043328
        ),
        cost_estimate=pl.CostEstimate(
            flops=rows * RANK * units * 6,
            bytes_accessed=units * RANK * 6,
            transcendentals=rows * units,
        ),
        name="layer",
    )(
        attended,
        residual,
        gain,
        router,
        select,
        first_at,
        second_at,
        named,
        proj_weight,
        near,
        u_gate_up,
        v_gate_up,
        u_down,
        v_down,
    )
    return out


def per_device(
    queries,
    keys,
    values,
    residual,
    proj_weight,
    norm_gain,
    router,
    expert_ids,
    u_gate_up,
    v_gate_up,
    u_down,
    v_down,
):
    attended, near = attention(queries, keys, values, proj_weight)
    expert_range = jnp.arange(EXPERTS, dtype=jnp.int32)
    member = (expert_ids[:, :, None] == expert_range).astype(jnp.bfloat16)
    tokens = jnp.arange(TOK_DEV, dtype=jnp.int32)
    before = jnp.dot(
        (tokens[:, None] > tokens[None, :]).astype(jnp.bfloat16),
        member[:, 0] + member[:, 1],
        preferred_element_type=jnp.float32,
    )
    slot = jnp.sum(member.astype(jnp.float32) * before[:, None, :], axis=-1).astype(jnp.int32)
    past = expert_ids + (EXPERTS * MAIN - MAIN) + slot
    dest = jnp.where(slot < MAIN, expert_ids * MAIN + slot, past)
    places = jnp.arange(EXPERTS * MAIN + PAD, dtype=jnp.int32)
    first_at = (dest[:, 0:1] == places[None, :]).astype(jnp.bfloat16)
    second_at = (dest[:, 1:2] == places[None, :]).astype(jnp.bfloat16)
    select = (
        (dest[:, 0][None, :] == places[:, None]) | (dest[:, 1][None, :] == places[:, None])
    ).astype(jnp.bfloat16)
    named = (expert_ids.T[:, :, None] == expert_range).astype(jnp.float32)
    return layer(
        attended,
        residual,
        norm_gain.astype(jnp.float32)[None, :],
        router.T,
        select,
        first_at,
        second_at,
        named,
        (proj_weight, near, u_gate_up, v_gate_up, u_down, v_down),
    )


def solution(mesh):
    in_specs = (
        P(("seq", "exp"), None),
        P(("seq", "exp"), None),
        P(("seq", "exp"), None),
        P(("seq", "exp"), None),
        P("seq", "exp"),
        P(),
        P(),
        P(("seq", "exp"), None),
        P("exp", None, None),
        P("exp", None, None, None),
        P("exp", None, None),
        P("exp", None, None),
    )
    out_specs = P(("seq", "exp"), None)
    return jax.shard_map(
        per_device, mesh=mesh, in_specs=in_specs, out_specs=out_specs, check_vma=False
    )
```

```python
import functools

import jax
import jax.numpy as jnp
from jax import lax
from jax.experimental import pallas as pl
from jax.experimental.pallas import tpu as pltpu
from jax.sharding import PartitionSpec as P

D = 6144
HEADS = 24
KV_HEADS = 4
HEAD_DIM = 128
EXPERTS = 8
RANK = 512
TOK_DEV = 128
CAP = 33


EPS = 1e-05
LOG2_E = 1.4426950408889634


MAIN = CAP // 16 * 16
PAD = 16
PIECE = 384
AHEAD = 2


def flipped(index, bits):
    bit = 1
    while bit <= bits:
        if bits & bit:
            index = index + bit * (1 - 2 * ((index // bit) % 2))
        bit *= 2
    return index


def at(**place):
    return {"device_id": place, "device_id_type": pl.DeviceIdType.MESH}


def greet(seq_count, exp_count):
    seq, exp = lax.axis_index("seq"), lax.axis_index("exp")
    barrier = pltpu.get_barrier_semaphore()
    for d in range(1, exp_count):
        pl.semaphore_signal(barrier, inc=1, **at(exp=flipped(exp, d)))
    for d in range(1, seq_count):
        for c in range(2):
            pl.semaphore_signal(
                barrier, inc=1, **at(seq=flipped(seq, d), exp=flipped(exp, c))
            )
    return barrier, exp_count - 1 + 2 * (seq_count - 1)


MAIN = CAP // 16 * 16
PAD = 16
PIECE = 384
AHEAD = 2


def flipped(index, bits):
    bit = 1
    while bit <= bits:
        if bits & bit:
            index = index + bit * (1 - 2 * ((index // bit) % 2))
        bit *= 2
    return index


def at(**place):
    return {"device_id": place, "device_id_type": pl.DeviceIdType.MESH}


def greet(seq_count, exp_count):
    seq, exp = lax.axis_index("seq"), lax.axis_index("exp")
    barrier = pltpu.get_barrier_semaphore()
    for d in range(1, exp_count):
        pl.semaphore_signal(barrier, inc=1, **at(exp=flipped(exp, d)))
    for d in range(1, seq_count):
        for c in range(2):
            pl.semaphore_signal(
                barrier, inc=1, **at(seq=flipped(seq, d), exp=flipped(exp, c))
            )
    return barrier, exp_count - 1 + 2 * (seq_count - 1)


def attention_kernel(
    seq_count,
    exp_count,
    q_ref,
    k_ref,
    v_ref,
    w_hbm,
    out_ref,
    near_hbm,
    q_all,
    kv_all,
    in_send,
    in_recv,
    q_send,
    q_recv,
    kv_send,
    kv_recv,
    w_send,
    w_recv,
    out_send,
    out_recv,
):
    seq, exp = lax.axis_index("seq"), lax.axis_index("exp")
    chips = exp_count // 2
    chip, core = exp // 2, exp % 2
    heads = HEADS // seq_count
    width = heads * HEAD_DIM
    shares = max(1, seq_count // KV_HEADS)
    barrier, greetings = greet(seq_count, exp_count)
    own = pl.ds(pl.multiple_of((seq // shares) * HEAD_DIM, HEAD_DIM), HEAD_DIM)
    kv_all[exp, seq, :, :HEAD_DIM] = k_ref[:, own]
    kv_all[exp, seq, :, HEAD_DIM:] = v_ref[:, own]
    q_all[seq] = q_ref[:, pl.ds(pl.multiple_of(seq * width, width), width)]
    pl.semaphore_wait(barrier, greetings)

    def kv_copy(half, peer, block):
        ref = (k_ref, v_ref)[half]
        head = pl.ds(pl.multiple_of((peer // shares) * HEAD_DIM, HEAD_DIM), HEAD_DIM)
        return pltpu.make_async_remote_copy(
            src_ref=ref.at[:, head],
            dst_ref=kv_all.at[exp, block, :, pl.ds(half * HEAD_DIM, HEAD_DIM)],
            send_sem=in_send.at[half, peer],
            recv_sem=in_recv.at[half, block],
            **at(seq=peer),
        )

    def q_copy(peer, block):
        return pltpu.make_async_remote_copy(
            src_ref=q_ref.at[:, pl.ds(pl.multiple_of(peer * width, width), width)],
            dst_ref=q_all.at[block],
            send_sem=q_send.at[peer],
            recv_sem=q_recv.at[block],
            **at(seq=peer),
        )

    for d in range(1, seq_count):
        for half in range(2):
            kv_copy(half, flipped(seq, d), seq).start()
    for d in range(1, seq_count):
        q_copy(flipped(seq, d), seq).start()

    def pass_on(way, block, target):
        return pltpu.make_async_remote_copy(
            src_ref=kv_all.at[block],
            dst_ref=kv_all.at[block],
            send_sem=kv_send.at[way, block],
            recv_sem=kv_recv.at[block],
            **at(exp=target),
        )

    cut_rows = w_hbm.shape[0] // 2
    sub = w_hbm.shape[1] // PIECE

    def weight(way, target, u):
        h = sub - 1 - u // 2 if way == 0 else u // 2
        rows = pl.ds((u % 2) * cut_rows, cut_rows)
        return pltpu.make_async_remote_copy(
            src_ref=w_hbm.at[rows, pl.ds(h * PIECE, PIECE)],
            dst_ref=near_hbm.at[way, h, rows],
            send_sem=w_send.at[way, u],
            recv_sem=w_recv.at[way, u],
            **at(exp=target),
        )

    def weights(low, high):
        @pl.when(chip + 1 < chips)
        def _():
            for u in range(low, high):
                weight(0, exp + 2, u).start()

        @pl.when(chip >= 1)
        def _():
            for u in range(low, high):
                weight(1, exp - 2, u).start()

    weights(0, 1)

    partner = flipped(exp, 1)

    def spread(block, up, down, act):
        if up:

            @pl.when(chip + 1 < chips)
            def _():
                act(pass_on(0, block, exp + 2))

        if down:

            @pl.when(chip >= 1)
            def _():
                act(pass_on(1, block, exp - 2))

        act(pass_on(2, block, partner))

    def start(copy):
        copy.start()

    def sent(copy):
        copy.wait_send()

    for d in range(1, seq_count):
        for half in range(2):
            peer = flipped(seq, d)
            kv_copy(half, peer, peer).wait_recv()
    spread(exp, True, True, start)

    def relay(act, wait):
        for hop in range(1, chips):
            below, above = exp - 2 * hop, exp + 2 * hop

            @pl.when(chip >= hop)
            def _():
                if wait:
                    pass_on(2, below, partner).wait_recv()
                spread(below, True, False, act)

            @pl.when(chip + hop < chips)
            def _():
                if wait:
                    pass_on(2, above, partner).wait_recv()
                spread(above, False, True, act)

    relay(start, True)

    weights(1, 2 * sub)

    for other in range(chips):
        pass_on(2, 2 * other + 1 - core, partner).wait_recv()
    for d in range(1, seq_count):
        peer = flipped(seq, d)
        q_copy(peer, peer).wait_recv()

    parts = max(1, exp_count * TOK_DEV // 512)
    span = exp_count // parts
    chunk = span * TOK_DEV
    rows = heads * TOK_DEV

    def attend(block, unused):
        query = jnp.concatenate(
            [q_all[block, :, h * HEAD_DIM : (h + 1) * HEAD_DIM] for h in range(heads)], axis=0
        )

        def step(index, carried, masked):
            row_max, row_sum, weighted = carried
            held = kv_all[pl.ds((index % parts) * span, span), index // parts]
            held = held.reshape(chunk, 2 * HEAD_DIM)
            scores = lax.dot_general(
                query,
                held[:, :HEAD_DIM],
                (((1,), (1,)), ((), ())),
                preferred_element_type=jnp.float32,
            ) * (HEAD_DIM ** (-0.5) * LOG2_E)
            if masked:
                offset = (exp % span) * TOK_DEV
                mine = lax.broadcasted_iota(jnp.int32, (rows, chunk), 0) % TOK_DEV + offset
                other = lax.broadcasted_iota(jnp.int32, (rows, chunk), 1)
                scores = jnp.where(other <= mine, scores, -jnp.inf)
            new_max = jnp.maximum(row_max, jnp.max(scores, axis=-1, keepdims=True))
            fading = jnp.exp2(row_max - new_max)
            terms = jnp.exp2(scores - new_max)
            row_sum = row_sum * fading + jnp.sum(terms, axis=-1, keepdims=True)
            update = jnp.dot(
                terms.astype(jnp.bfloat16), held[:, HEAD_DIM:], preferred_element_type=jnp.float32
            )
            return new_max, row_sum, weighted * fading + update

        carried = (
            jnp.full((rows, 1), -1e30, jnp.float32),
            jnp.zeros((rows, 1), jnp.float32),
            jnp.zeros((rows, HEAD_DIM), jnp.float32),
        )
        last = block * parts + exp // span
        carried = lax.fori_loop(0, last, lambda index, now: step(index, now, False), carried)
        row_max, row_sum, weighted = step(last, carried, True)
        result = (weighted / row_sum).astype(jnp.bfloat16)
        for h in range(heads):
            out_ref[core, block, :, h * HEAD_DIM : (h + 1) * HEAD_DIM] = result[
                h * TOK_DEV : (h + 1) * TOK_DEV
            ]
        share(core, block).start()
        return unused

    def share(slot, block):
        return pltpu.make_async_remote_copy(
            src_ref=out_ref.at[slot, block],
            dst_ref=out_ref.at[slot, block],
            send_sem=out_send.at[block],
            recv_sem=out_recv.at[block],
            **at(exp=partner),
        )

    lax.fori_loop(0, seq_count, attend, 0)
    for d in range(1, seq_count):
        peer = flipped(seq, d)
        for half in range(2):
            kv_copy(half, peer, peer).wait_send()
        q_copy(peer, peer).wait_send()
    spread(exp, True, True, sent)
    relay(sent, False)
    for block in range(seq_count):
        share(core, block).wait_send()
        share(1 - core, block).wait_recv()

    @pl.when(chip + 1 < chips)
    def _():
        for u in range(2 * sub):
            weight(0, exp + 2, u).wait_send()
            weight(1, partner, u).wait_recv()

    @pl.when(chip >= 1)
    def _():
        for u in range(2 * sub):
            weight(1, exp - 2, u).wait_send()
            weight(0, partner, u).wait_recv()


def attention(queries, keys, values, proj_weight):
    seq_count, exp_count = lax.axis_size("seq"), lax.axis_size("exp")
    width = HEADS // seq_count * HEAD_DIM
    blocks = (seq_count, TOK_DEV, width)
    pairs = HEADS // seq_count * seq_count * TOK_DEV * exp_count * seq_count * TOK_DEV // 2
    vmem = pl.BlockSpec(memory_space=pltpu.VMEM)
    anywhere = pl.BlockSpec(memory_space=pl.ANY)
    dma = pltpu.SemaphoreType.DMA
    return pl.pallas_call(
        functools.partial(attention_kernel, seq_count, exp_count),
        out_shape=(
            jax.ShapeDtypeStruct((2, *blocks), jnp.bfloat16),
            jax.ShapeDtypeStruct(
                (2, proj_weight.shape[1] // PIECE, proj_weight.shape[0], PIECE), jnp.bfloat16
            ),
        ),
        in_specs=[vmem, vmem, vmem, anywhere],
        out_specs=(vmem, anywhere),
        scratch_shapes=[
            pltpu.VMEM(blocks, jnp.bfloat16),
            pltpu.VMEM((exp_count, seq_count, TOK_DEV, 2 * HEAD_DIM), jnp.bfloat16),
            dma((2, seq_count)),
            dma((2, seq_count)),
            dma((seq_count,)),
            dma((seq_count,)),
            dma((3, exp_count)),
            dma((exp_count,)),
            dma((2, proj_weight.shape[1] // PIECE * 2)),
            dma((2, proj_weight.shape[1] // PIECE * 2)),
            dma((seq_count,)),
            dma((seq_count,)),
        ],
        compiler_params=pltpu.CompilerParams(
            collective_id=1, has_side_effects=True, vmem_limit_bytes=60 * 1024 * 1024
        ),
        cost_estimate=pl.CostEstimate(
            flops=pairs * 4 * HEAD_DIM, bytes_accessed=queries.size * 4, transcendentals=pairs
        ),
        name="attention",
    )(queries, keys, values, proj_weight)


def gather_lanes(ref, chunk, tiles):
    return jnp.concatenate([ref[chunk, :, t, :] for t in range(tiles)], axis=1)


def padded(rows):
    count = rows.shape[0]
    if count % PAD:
        rows = jnp.concatenate(
            [rows, jnp.zeros((PAD - count % PAD, rows.shape[1]), rows.dtype)], axis=0
        )
    return rows.astype(jnp.bfloat16)


def layer_kernel(
    seq_count,
    count,
    steps,
    depth,
    att_ref,
    res_ref,
    gain_ref,
    router_ref,
    sel_ref,
    first_ref,
    second_ref,
    named_ref,
    w_hbm,
    near_hbm,
    u_hbm,
    vg_hbm,
    ud_hbm,
    vd_hbm,
    out_ref,
    far_hbm,
    w_buf,
    part_send,
    part_recv,
    stream,
    u_buf,
    vg_buf,
    ud_buf,
    send,
    recv,
    back,
    send_x,
    recv_x,
    back_x,
    rank_sum,
    rank_in,
    square,
    token,
    mix_both,
    swap,
    swap_x,
    w_sem,
    load_sem,
    far_send,
    far_recv,
    part_send_sem,
    part_recv_sem,
    send_sem,
    recv_sem,
    send_x_sem,
    recv_x_sem,
    swap_sem,
):
    seq, me = lax.axis_index("seq"), lax.axis_index("exp")
    chips = count // 2
    chip, core = me // 2, me % 2
    pieces = count // EXPERTS
    piece_width = D // pieces
    block = D // count
    sub = block // PIECE
    width = 2 * PIECE
    tiles = width // 128
    total = chips * sub
    local = total // pieces
    unit = vg_buf.shape[-1]
    mine = me % pieces
    early = chip < (chips + 1) // 2
    rows_in = TOK_DEV * 2 * seq_count
    barrier, greetings = greet(seq_count, count)

    def chunk_of(i):
        return jnp.where(early, i, total - 1 - i)

    def columns(g):
        first = (g // sub) * 2 * block + (g % sub) * PIECE
        return first, first + block

    def span(start):
        return pl.ds(pl.multiple_of(start, 128), PIECE)

    def u_copies(l):
        return [
            pltpu.make_async_copy(
                u_hbm.at[0, pl.ds(pl.multiple_of(start - mine * piece_width, 128), PIECE)],
                u_buf.at[l, pl.ds(p * PIECE, PIECE)],
                w_sem.at[p, l],
            )
            for p, start in enumerate(columns(mine * local + l))
        ]

    def vd_copies(l):
        return [
            pltpu.make_async_copy(
                vd_hbm.at[0, :, span(start - mine * piece_width)],
                u_buf.at[l, pl.ds(0, RANK), pl.ds(p * PIECE, PIECE)],
                w_sem.at[2 + p, l],
            )
            for p, start in enumerate(columns(mine * local + l))
        ]

    def vg_copy(f):
        cols = pl.ds(pl.multiple_of(f * unit, unit), unit)
        return pltpu.make_async_copy(vg_hbm.at[0, :, :, cols], vg_buf.at[f % depth], w_sem.at[4, f])

    def ud_copy(f):
        rows = pl.ds(pl.multiple_of(f * unit, unit), unit)
        return pltpu.make_async_copy(ud_hbm.at[0, rows], ud_buf.at[f % depth], w_sem.at[5, f])

    cut_rows = w_hbm.shape[0] // 2
    units = 2 * sub

    def part_of(way, u):
        h = sub - 1 - u // 2 if way == 0 else u // 2
        return h, pl.ds((u % 2) * cut_rows, cut_rows), u % 2

    def weight_hop(way, origin, u, near):
        h, rows, r = part_of(way, u)
        target = far_hbm.at[origin, h, rows]
        return pltpu.make_async_remote_copy(
            src_ref=near_hbm.at[way, h, rows] if near else target,
            dst_ref=target,
            send_sem=far_send.at[way, origin, h, r],
            recv_sem=far_recv.at[origin, h, r],
            **at(exp=me + 2 if way == 0 else me - 2),
        )

    def far_arrival(origin, h, r):
        target = far_hbm.at[origin, h, pl.ds(r * cut_rows, cut_rows)]
        return pltpu.make_async_remote_copy(
            src_ref=target,
            dst_ref=target,
            send_sem=far_send.at[0, origin, h, r],
            recv_sem=far_recv.at[origin, h, r],
            **at(exp=flipped(me, 1)),
        )

    def pump(j, act, wait):
        distance, u = j // units, j % units
        below, above = chip - distance, chip + distance

        @pl.when((below >= 0) & (chip + 1 < chips))
        def _():
            if wait and distance > 1:
                h, _, r = part_of(0, u)
                far_arrival(below, h, r).wait_recv()
            act(weight_hop(0, below, u, distance == 1))

        @pl.when((above < chips) & (chip >= 1))
        def _():
            if wait and distance > 1:
                h, _, r = part_of(1, u)
                far_arrival(above, h, r).wait_recv()
            act(weight_hop(1, above, u, distance == 1))

    pump_count = (chips - 1) * units

    def start(copy):
        copy.start()

    def sent(copy):
        copy.wait_send()

    def load(i):
        g = chunk_of(i)
        origin, h = g // sub, g % sub

        @pl.when(origin == chip)
        def _():
            pltpu.make_async_copy(w_hbm.at[:, span(h * PIECE)], w_buf, load_sem).start()

        @pl.when(origin == chip - 1)
        def _():
            pltpu.make_async_copy(near_hbm.at[0, h], w_buf, load_sem).start()

        @pl.when(origin == chip + 1)
        def _():
            pltpu.make_async_copy(near_hbm.at[1, h], w_buf, load_sem).start()

        @pl.when((origin >= chip + 2) | (origin <= chip - 2))
        def _():
            @pl.when(((origin > chip) & (chip == 0)) | ((origin < chip) & (chip == chips - 1)))
            def _():
                for r in range(2):
                    far_arrival(origin, h, r).wait_recv()

            pltpu.make_async_copy(far_hbm.at[origin, h], w_buf, load_sem).start()

        pltpu.make_async_copy(near_hbm.at[0, h], w_buf, load_sem).wait()

    def part_copy(i, d, t, block_from, core_from):
        peer, exp = flipped(seq, d), flipped(me, t)
        return pltpu.make_async_remote_copy(
            src_ref=part_send.at[i % (AHEAD + 1), exp % 2, peer],
            dst_ref=part_recv.at[i, core_from, block_from],
            send_sem=part_send_sem.at[i % (AHEAD + 1), exp % 2, peer],
            recv_sem=part_recv_sem.at[i, core_from, block_from],
            **at(seq=peer, exp=exp),
        )

    targets = [(d, t) for d in range(seq_count) for t in range(2) if d or t]

    def parts_sent(i):
        for d, t in targets:
            part_copy(i, d, t, seq, core).wait_send()

    def project(i):
        load(i)
        part = jnp.dot(
            att_ref[...].reshape(rows_in, att_ref.shape[-1]),
            w_buf[...],
            preferred_element_type=jnp.float32,
        )
        slot = i % (AHEAD + 1)
        part_send[slot] = part.astype(jnp.bfloat16).reshape(2, seq_count, TOK_DEV, PIECE)
        for d, t in targets:
            part_copy(i, d, t, seq, core).start()
        part_recv[i, core, seq] = part_send[slot, core, seq]

    def copies(phase, l, peer, slot, into, into_x):
        main = pltpu.make_async_remote_copy(
            src_ref=send.at[l, peer],
            dst_ref=into.at[l, slot],
            send_sem=send_sem.at[phase, l, peer],
            recv_sem=recv_sem.at[phase, l, slot],
            **at(exp=peer),
        )
        extra = pltpu.make_async_remote_copy(
            src_ref=send_x.at[l, peer],
            dst_ref=into_x.at[l, slot],
            send_sem=send_x_sem.at[phase, l, peer],
            recv_sem=recv_x_sem.at[phase, l, slot],
            **at(exp=peer),
        )
        return main, extra

    def send_chunk(phase, l, piece, into, into_x):
        for d in range(1, count):
            peer = flipped(me, d)

            def go():
                for copy in copies(phase, l, peer, me, into, into_x):
                    copy.start()

            if piece is None or pieces == 1:
                go()
            else:
                pl.when(peer % pieces == piece)(go)

        def keep():
            into[l, me] = send[l, me]
            into_x[l, me] = send_x[l, me]

        if piece is None or pieces == 1:
            keep()
        else:
            pl.when(mine == piece)(keep)

    def wait_sent(phase, l, into, into_x):
        for d in range(1, count):
            peer = flipped(me, d)
            for copy in copies(phase, l, peer, peer, into, into_x):
                copy.wait_send()

    def wait_got(phase, l, into, into_x, peers):
        for peer in peers:

            @pl.when(peer != me)
            def _():
                for copy in copies(phase, l, peer, peer, into, into_x):
                    copy.wait_recv()

    def finish(i):
        g = chunk_of(i)
        for d, t in targets:
            peer, exp = flipped(seq, d), flipped(me, t)
            part_copy(i, d, t, peer, exp % 2).wait_recv()
        halves = []
        for p, first in enumerate(columns(g)):
            update = part_recv[i, p, 0].astype(jnp.float32)
            for s in range(1, seq_count):
                update = update + part_recv[i, p, s].astype(jnp.float32)
            update = update.astype(jnp.bfloat16).astype(jnp.float32)
            value = res_ref[:, span(first)].astype(jnp.float32) + update
            stream[g, :, p * PIECE : (p + 1) * PIECE] = value
            token[0] += jnp.broadcast_to(
                jnp.sum(value * value, axis=-1, keepdims=True), (TOK_DEV, 128)
            )
            gained = (value * gain_ref[:, span(first)]).astype(jnp.bfloat16)
            token[1, :, :EXPERTS] += lax.dot_general(
                gained,
                router_ref[:, span(first)],
                (((1,), (1,)), ((), ())),
                preferred_element_type=jnp.float32,
            )
            halves.append(value.astype(jnp.bfloat16))
        rows = jnp.dot(
            sel_ref[...], jnp.concatenate(halves, axis=1), preferred_element_type=jnp.float32
        )
        piece, l = g // local, g % local
        for k in range(EXPERTS):
            send[l, k * pieces + piece] = rows[k * MAIN : (k + 1) * MAIN].astype(jnp.bfloat16)
        extra = rows[EXPERTS * MAIN : EXPERTS * MAIN + EXPERTS]
        for t in range(tiles):
            lanes = extra[:, t * 128 : (t + 1) * 128]
            if pieces == 1:
                send_x[l, :, t, :] = lanes
            else:
                for k in range(EXPERTS):
                    send_x[l, k * pieces + piece, t : t + 1, :] = lanes[k : k + 1]
        send_chunk(0, l, piece, recv, recv_x)

    def weights_in():
        for l in range(local):
            for copy in u_copies(l):
                copy.start()
        for f in range(min(depth, steps)):
            vg_copy(f).start()
            ud_copy(f).start()

    pl.semaphore_wait(barrier, greetings)
    for j in range(units, 2 * units):
        pump(j, start, True)
    rest = list(range(2 * units, pump_count))
    if len(rest) > 4:
        for j in rest:
            pump(j, start, True)
        rest = []
    token[...] = jnp.zeros_like(token)
    square[...] = jnp.zeros_like(square)
    rank_sum[...] = jnp.zeros_like(rank_sum)

    def first_half(i, carried):
        @pl.when(i < total)
        def _():
            @pl.when(i > AHEAD)
            def _():
                parts_sent(i - AHEAD - 1)

            project(i)

        @pl.when(i == min(AHEAD, total - 1))
        def _():
            weights_in()

        @pl.when(i == AHEAD)
        def _():
            for j in rest:
                pump(j, start, True)

        @pl.when(i >= AHEAD)
        def _():
            finish(i - AHEAD)

        return carried

    lax.fori_loop(0, total + AHEAD, first_half, 0)
    for i in range(total - AHEAD - 1, total):
        parts_sent(i)

    split = 2 * ((chips + 1) // 2)
    main_rows = count * MAIN

    def spread_gain(l):
        return jnp.concatenate(
            [gain_ref[:, span(start)] for start in columns(mine * local + l)], axis=1
        )

    def first_factor(t, carried):
        for low, high, l in ((0, split, t), (split, count, local - 1 - t)):
            wait_got(0, l, recv, recv_x, range(low, high))
            held = recv[l, low:high].reshape((high - low) * MAIN, width).astype(jnp.float32)
            extra = jnp.concatenate([recv_x[l, low:high, k, :] for k in range(tiles)], axis=1)
            fill = [jnp.zeros((low, width), jnp.float32)] if low else []
            rest = PAD - high
            fill += [extra] + ([jnp.zeros((rest, width), jnp.float32)] if rest else [])
            extra = jnp.concatenate(fill, axis=0) if len(fill) > 1 else extra
            rows = jnp.concatenate([held, extra], axis=0)
            squares = jnp.sum(rows * rows, axis=-1, keepdims=True)
            squares = jnp.broadcast_to(squares, (rows.shape[0], 128))
            gained = (rows * spread_gain(l)).astype(jnp.bfloat16)
            product = jnp.dot(gained, u_buf[l], preferred_element_type=jnp.float32)
            size = (high - low) * MAIN
            here = slice(low * MAIN, high * MAIN)
            square[here] += squares[:size]
            square[main_rows:] += squares[size:]
            rank_sum[here] += product[:size]
            rank_sum[main_rows:] += product[size:]
        return carried

    for l in range(local):
        for copy in u_copies(l):
            copy.wait()
    lax.fori_loop(0, local, first_factor, 0)
    for l in range(local):
        for copy in vd_copies(l):
            copy.start()

    def exchange(source, target, slot, bit):
        copy = pltpu.make_async_remote_copy(
            src_ref=source,
            dst_ref=target,
            send_sem=swap_sem.at[slot, 0],
            recv_sem=swap_sem.at[slot, 1],
            **at(exp=flipped(me, bit)),
        )
        copy.start()
        copy.wait()

    def add_pieces(slot, columns, with_square):
        bit = 1
        while bit < pieces:
            swap[slot, 0, :, :columns] = rank_sum[:, :columns].astype(jnp.bfloat16)
            exchange(swap.at[slot, 0], swap.at[slot, 1], 2 * slot, bit)
            rank_sum[:, :columns] += swap[slot, 1, :, :columns].astype(jnp.float32)
            if with_square:
                swap_x[slot, 0] = square[...]
                exchange(swap_x.at[slot, 0], swap_x.at[slot, 1], 2 * slot + 1, bit)
                square[...] += swap_x[slot, 1]
            bit *= 2
            slot += 1
        return slot

    slot = add_pieces(0, 2 * RANK, True)
    scale = lax.rsqrt(square[:, 0:1] * (1.0 / D) + EPS)
    rank_in[...] = (rank_sum[...] * scale).astype(jnp.bfloat16)
    rank_sum[:, :RANK] = jnp.zeros((rank_sum.shape[0], RANK), jnp.float32)

    def middle(f, carried):
        vg_copy(f).wait()
        ud_copy(f).wait()
        place = f % depth
        gate = jnp.dot(rank_in[:, :RANK], vg_buf[place, 0], preferred_element_type=jnp.float32)
        up = jnp.dot(rank_in[:, RANK:], vg_buf[place, 1], preferred_element_type=jnp.float32)
        hidden = (gate / (1.0 + jnp.exp(-gate)) * up).astype(jnp.bfloat16)
        rank_sum[:, :RANK] += jnp.dot(hidden, ud_buf[place], preferred_element_type=jnp.float32)

        @pl.when(f + depth < steps)
        def _():
            vg_copy(f + depth).start()
            ud_copy(f + depth).start()

        return carried

    lax.fori_loop(0, steps, middle, 0)
    add_pieces(slot, RANK, False)
    rank_in[:, :RANK] = rank_sum[:, :RANK].astype(jnp.bfloat16)

    def last_factor(l, carried):
        for copy in vd_copies(l):
            copy.wait()
        wait_sent(0, l, recv, recv_x)
        rows = jnp.dot(
            rank_in[:, :RANK], u_buf[l, :RANK, :width], preferred_element_type=jnp.float32
        )
        for k in range(count):
            send[l, k] = rows[k * MAIN : (k + 1) * MAIN].astype(jnp.bfloat16)
        extra = rows[main_rows : main_rows + count]
        for t in range(tiles):
            send_x[l, :, t, :] = extra[:, t * 128 : (t + 1) * 128]
        send_chunk(1, l, None, back, back_x)
        return carried

    lax.fori_loop(0, local, last_factor, 0)

    logits = token[1, :, :EXPERTS] * lax.rsqrt(token[0, :, 0:1] * (1.0 / D) + EPS)
    first = jnp.sum(logits * named_ref[0], axis=-1, keepdims=True)
    second = jnp.sum(logits * named_ref[1], axis=-1, keepdims=True)
    mix = first_ref[...].astype(jnp.float32) / (1.0 + jnp.exp(second - first)) + second_ref[
        ...
    ].astype(jnp.float32) / (1.0 + jnp.exp(first - second))
    mix_high = mix.astype(jnp.bfloat16)
    mix_both[:TOK_DEV] = mix_high
    mix_both[TOK_DEV:] = (mix - mix_high.astype(jnp.float32)).astype(jnp.bfloat16)

    def combine(l, carried):
        wait_got(1, l, back, back_x, range(count))
        for piece in range(pieces):
            g = piece * local + l
            rows = back[l].reshape(EXPERTS, pieces, MAIN, width)[:, piece]
            extra = gather_lanes(back_x, l, tiles).reshape(EXPERTS, pieces, width)[:, piece]
            rows = jnp.concatenate([rows.reshape(EXPERTS * MAIN, width), padded(extra)], axis=0)
            both = jnp.dot(mix_both[...], rows, preferred_element_type=jnp.float32)
            result = (stream[g] + both[:TOK_DEV] + both[TOK_DEV:]).astype(jnp.bfloat16)
            for p, first in enumerate(columns(g)):
                out_ref[:, span(first)] = result[:, p * PIECE : (p + 1) * PIECE]
        return carried

    lax.fori_loop(0, local, combine, 0)

    def drain(l, carried):
        wait_sent(1, l, back, back_x)
        return carried

    lax.fori_loop(0, local, drain, 0)
    for j in range(units, pump_count):
        pump(j, sent, False)


def layer(attended, residual, gain, router, select, first_at, second_at, named, weights):
    proj_weight, near, u_gate_up, v_gate_up, u_down, v_down = weights
    seq_count, count = lax.axis_size("seq"), lax.axis_size("exp")
    pieces = count // EXPERTS
    sub = D // count // PIECE
    total = count // 2 * sub
    local = total // pieces
    width = 2 * PIECE
    units = u_down.shape[1]
    unit = min(1024, units)
    steps = units // unit
    depth = min(5, max(1, steps - 2))
    rows = count * MAIN + PAD
    swaps = max(1, 2 * (pieces.bit_length() - 1))
    depth_in = proj_weight.shape[0]
    vmem = pl.BlockSpec(memory_space=pltpu.VMEM)
    anywhere = pl.BlockSpec(memory_space=pl.ANY)
    dma = pltpu.SemaphoreType.DMA
    half, full = jnp.bfloat16, jnp.float32
    block = (local, count, MAIN, width)
    block_x = (local, count, width // 128, 128)
    many = pieces > 1
    out, _ = pl.pallas_call(
        functools.partial(layer_kernel, seq_count, count, steps, depth),
        out_shape=(
            jax.ShapeDtypeStruct((TOK_DEV, D), half),
            jax.ShapeDtypeStruct((count // 2, sub, depth_in, PIECE), half),
        ),
        in_specs=[vmem] * 8 + [anywhere] * 6,
        out_specs=(vmem, anywhere),
        scratch_shapes=[
            pltpu.VMEM((depth_in, PIECE), half),
            pltpu.VMEM((AHEAD + 1, 2, seq_count, TOK_DEV, PIECE), half),
            pltpu.VMEM((total, 2, seq_count, TOK_DEV, PIECE), half),
            pltpu.VMEM((total, TOK_DEV, width), full),
            pltpu.VMEM((local, width, 2 * RANK), half),
            pltpu.VMEM((depth, 2, RANK, unit), half),
            pltpu.VMEM((depth, unit, RANK), half),
            pltpu.VMEM(block, half),
            pltpu.VMEM(block, half),
            pltpu.VMEM(block, half),
            pltpu.VMEM(block_x, full),
            pltpu.VMEM(block_x, full),
            pltpu.VMEM(block_x, full),
            pltpu.VMEM((rows, 2 * RANK), full),
            pltpu.VMEM((rows, 2 * RANK), half),
            pltpu.VMEM((rows, 128), full),
            pltpu.VMEM((2, TOK_DEV, 128), full),
            pltpu.VMEM((2 * TOK_DEV, select.shape[0]), half),
            pltpu.VMEM((swaps, 2, rows, 2 * RANK) if many else (1, 2, 16, 128), half),
            pltpu.VMEM((swaps, 2, rows, 128) if many else (1, 2, 8, 128), full),
            dma((6, max(local, steps))),
            dma(()),
            dma((2, count // 2, sub, 2)),
            dma((count // 2, sub, 2)),
            dma((AHEAD + 1, 2, seq_count)),
            dma((total, 2, seq_count)),
            dma((2, local, count)),
            dma((2, local, count)),
            dma((2, local, count)),
            dma((2, local, count)),
            dma((2 * swaps, 2)),
        ],
        compiler_params=pltpu.CompilerParams(
            collective_id=0, has_side_effects=True, vmem_limit_bytes=67043328
        ),
        cost_estimate=pl.CostEstimate(
            flops=rows * RANK * units * 6,
            bytes_accessed=units * RANK * 6,
            transcendentals=rows * units,
        ),
        name="layer",
    )(
        attended,
        residual,
        gain,
        router,
        select,
        first_at,
        second_at,
        named,
        proj_weight,
        near,
        u_gate_up,
        v_gate_up,
        u_down,
        v_down,
    )
    return out


def per_device(
    queries,
    keys,
    values,
    residual,
    proj_weight,
    norm_gain,
    router,
    expert_ids,
    u_gate_up,
    v_gate_up,
    u_down,
    v_down,
):
    attended, near = attention(queries, keys, values, proj_weight)
    expert_range = jnp.arange(EXPERTS, dtype=jnp.int32)
    member = (expert_ids[:, :, None] == expert_range).astype(jnp.bfloat16)
    tokens = jnp.arange(TOK_DEV, dtype=jnp.int32)
    before = jnp.dot(
        (tokens[:, None] > tokens[None, :]).astype(jnp.bfloat16),
        member[:, 0] + member[:, 1],
        preferred_element_type=jnp.float32,
    )
    slot = jnp.sum(member.astype(jnp.float32) * before[:, None, :], axis=-1).astype(jnp.int32)
    past = expert_ids + (EXPERTS * MAIN - MAIN) + slot
    dest = jnp.where(slot < MAIN, expert_ids * MAIN + slot, past)
    places = jnp.arange(EXPERTS * MAIN + PAD, dtype=jnp.int32)
    first_at = (dest[:, 0:1] == places[None, :]).astype(jnp.bfloat16)
    second_at = (dest[:, 1:2] == places[None, :]).astype(jnp.bfloat16)
    select = (
        (dest[:, 0][None, :] == places[:, None]) | (dest[:, 1][None, :] == places[:, None])
    ).astype(jnp.bfloat16)
    named = (expert_ids.T[:, :, None] == expert_range).astype(jnp.float32)
    return layer(
        attended,
        residual,
        norm_gain.astype(jnp.float32)[None, :],
        router.T,
        select,
        first_at,
        second_at,
        named,
        (proj_weight, near, u_gate_up, v_gate_up, u_down, v_down),
    )


def solution(mesh):
    in_specs = (
        P(("seq", "exp"), None),
        P(("seq", "exp"), None),
        P(("seq", "exp"), None),
        P(("seq", "exp"), None),
        P("seq", "exp"),
        P(),
        P(),
        P(("seq", "exp"), None),
        P("exp", None, None),
        P("exp", None, None, None),
        P("exp", None, None),
        P("exp", None, None),
    )
    out_specs = P(("seq", "exp"), None)
    return jax.shard_map(
        per_device, mesh=mesh, in_specs=in_specs, out_specs=out_specs, check_vma=False
    )
```
